256 devices in a mesh: wide: 64 (over z, x, core), narrow: 4 (over y).
Axes of the slice: x: 4, y: 4, z: 8, core: 2. Of those that a mesh axis runs over, the one named last changes fastest.
Arguments:
- query_states: bfloat16 [4096, 8192], P('wide', 'narrow'), may hold values from -8 to 8
- key_states: bfloat16 [4096, 8192], P('wide', 'narrow'), may hold values from -8 to 8
- value_states: bfloat16 [4096, 8192], P('wide', 'narrow'), may hold values from -6 to 6
- cache_keys: bfloat16 [4096, 1024], P('wide'), may hold values from -8 to 8
- cache_values: bfloat16 [4096, 1024], P('wide'), may hold values from -6 to 6
- gate_fast: bfloat16 [8, 512, 512], P('narrow'), may hold values from -0.25 to 0.25
- lift_fast: bfloat16 [8, 512, 512], P('narrow'), may hold values from -0.25 to 0.25
- down_fast: bfloat16 [8, 512, 512], P('narrow'), may hold values from -0.25 to 0.25
- token_rates: float32 [8, 8192], replicated, may hold values from 0.05 to 1
Outputs:
- attended: bfloat16 [4096, 8192], P('wide', 'narrow')
- recalled: bfloat16 [4096, 8192], P('wide', 'narrow')
The draws below stay inside these ranges and needn't reach their ends.
All inputs are finite; a program needn't handle non-finite values.
Results may differ from the reference program's by a relative error of at most 0.0094.
Values may be sent and summed in bfloat16 or wider, within the bound.
A program may use at most 64 MiB of HBM per device.

```python
import math
import jax
import jax.numpy as jnp
from jax import lax

FAST_HEADS = 8
FD = 512
FH = 512
D = 4096
HEAD_SIZE = 128
HEADS = 32
WINDOW = 1024
TOKENS = 8192
NS_ITERS = 2


def background(key):
    drawn = jnp.clip(1.5 * jax.random.normal(key, (D, TOKENS), jnp.float32), -8.0, 8.0)
    return drawn


def draw_query_states(key, part):
    drawn = background(jax.random.fold_in(key, 11))
    return drawn.astype(jnp.bfloat16)


def draw_key_states(key, part):
    drawn = background(jax.random.fold_in(key, 13))
    return drawn.astype(jnp.bfloat16)


def block_levels(rng, shape, shards, smallest, top_value):
    def one(dim, parts):
        draws = jax.random.uniform(jax.random.fold_in(jax.random.fold_in(rng, 6), dim), (parts,), jnp.float32, smallest / len(shards), top_value / len(shards))
        return jnp.repeat(jnp.exp(draws), shape[dim] // parts).reshape((-1,) + (1,) * (len(shape) - dim - 1))

    gain = one(*shards[0])
    for cut in shards[1:]:
        gain = gain * one(*cut)
    return gain


def scatter_about(key, shape, spread, limit, split=(), kind=jnp.bfloat16):
    entries = spread * jax.random.normal(key, shape, jnp.float32)
    if split:
        entries = entries * block_levels(key, shape, split, -0.22, 0.18)
    return jnp.clip(entries, -limit, limit).astype(kind)


def setup_inputs(seed: int = 0) -> dict:
    key_list = jax.random.split(jax.random.key(seed), 10)
    query_states = draw_query_states(jax.random.fold_in(key_list[9], 71), 0)
    key_states = draw_key_states(jax.random.fold_in(key_list[9], 71), 0)
    value_states = scatter_about(key_list[2], (D, TOKENS), 1.0, 6.0, ((0, 64), (1, 4)))
    cache_keys = scatter_about(key_list[3], (D, WINDOW), 1.5, 8.0, ((0, 64),))
    cache_values = scatter_about(key_list[4], (D, WINDOW), 1.0, 6.0, ((0, 64),))
    gate_fast = scatter_about(key_list[5], (FAST_HEADS, FH, FD), FD ** -0.5, 0.25, ((0, 4),))
    lift_fast = scatter_about(key_list[6], (FAST_HEADS, FH, FD), FD ** -0.5, 0.25, ((0, 4),))
    down_fast = scatter_about(key_list[7], (FAST_HEADS, FD, FH), FH ** -0.5, 0.25, ((0, 4),))
    token_rates = jnp.clip(jnp.exp(jax.random.uniform(key_list[8], (FAST_HEADS, TOKENS), jnp.float32, math.log(0.05), math.log(1.0))), 0.05, 1.0)
    return {"query_states": query_states, "key_states": key_states, "value_states": value_states, "cache_keys": cache_keys, "cache_values": cache_values, "gate_fast": gate_fast, "lift_fast": lift_fast, "down_fast": down_fast, "token_rates": token_rates}


EPS = 1e-06
COEF_A = 3.4445
COEF_B = -4.775
COEF_C = 2.0315

def stored(value):
    return lax.optimization_barrier(value.astype(jnp.bfloat16))

def attend_head(head_queries, head_keys, head_values):
    block_rows = min(512, TOKENS)
    block_count = TOKENS // block_rows
    key_span = WINDOW + block_rows
    scaling = 1.0 / math.sqrt(HEAD_SIZE)
    rows_at = jnp.arange(block_rows, dtype=jnp.int32)[:, None]
    cols_at = jnp.arange(key_span, dtype=jnp.int32)[None, :]
    visible = (cols_at > rows_at) & (cols_at <= rows_at + WINDOW)

    def one_block(block_index):
        offset = block_index * block_rows
        query_part = lax.dynamic_slice_in_dim(head_queries, offset, block_rows, 1)
        key_part = lax.dynamic_slice_in_dim(head_keys, offset, key_span, 1)
        value_part = lax.dynamic_slice_in_dim(head_values, offset, key_span, 1)
        scores = jnp.dot(query_part.T, key_part, preferred_element_type=jnp.float32) * scaling
        scores = jnp.where(visible, scores, -jnp.inf)
        highest = lax.optimization_barrier(jnp.max(scores, axis=1, keepdims=True))
        raised = jnp.exp(scores - highest)
        weights = (raised / lax.optimization_barrier(jnp.sum(raised, axis=1, keepdims=True))).astype(jnp.bfloat16)
        return jnp.dot(value_part, weights.T, preferred_element_type=jnp.float32).astype(jnp.bfloat16)
    blocks_out = lax.map(one_block, jnp.arange(block_count, dtype=jnp.int32))
    return jnp.transpose(blocks_out, (1, 0, 2)).reshape(HEAD_SIZE, TOKENS)

def orthogonal(gradient):
    rounded = stored(gradient)
    widened = rounded.astype(jnp.float32)
    norm_val = jnp.sqrt(jnp.sum(jnp.square(widened)) + EPS)
    current = stored(widened / norm_val)
    for sweep_index in range(NS_ITERS):
        gram_mat = jnp.dot(current.T, current, preferred_element_type=jnp.float32).astype(jnp.bfloat16)
        lifted = stored(jnp.dot(current, gram_mat, preferred_element_type=jnp.float32))
        current = stored(COEF_A * current.astype(jnp.float32) + COEF_B * lifted.astype(jnp.float32) + COEF_C * jnp.dot(lifted, gram_mat, preferred_element_type=jnp.float32))
    return current

def refreshed(weight, ortho):
    initial = weight.astype(jnp.float32)
    moved_rows = initial - ortho.astype(jnp.float32)
    wanted = jnp.sqrt(lax.optimization_barrier(jnp.mean(jnp.square(initial), axis=-1, keepdims=True)) + EPS)
    present = jnp.sqrt(lax.optimization_barrier(jnp.mean(jnp.square(moved_rows), axis=-1, keepdims=True)) + EPS)
    return (moved_rows * (wanted / present)).astype(jnp.bfloat16)

def reference(query_states, key_states, value_states, cache_keys, cache_values, gate_fast, lift_fast, down_fast, token_rates):
    ext_keys = jnp.concatenate([cache_keys, key_states], axis=1)
    ext_values = jnp.concatenate([cache_values, value_states], axis=1)

    def per_head(head_index):
        first_row = head_index * HEAD_SIZE
        return attend_head(lax.dynamic_slice_in_dim(query_states, first_row, HEAD_SIZE, 0), lax.dynamic_slice_in_dim(ext_keys, first_row, HEAD_SIZE, 0), lax.dynamic_slice_in_dim(ext_values, first_row, HEAD_SIZE, 0))
    attended = lax.map(per_head, jnp.arange(HEADS, dtype=jnp.int32)).reshape(D, TOKENS)

    def per_fast(head_index):
        first_row = head_index * FD
        query_fast = lax.dynamic_slice_in_dim(query_states, first_row, FD, 0)
        key_fast = lax.dynamic_slice_in_dim(key_states, first_row, FD, 0)
        value_fast = lax.dynamic_slice_in_dim(value_states, first_row, FD, 0)
        gate_weight = gate_fast[head_index]
        lift_weight = lift_fast[head_index]
        down_weight = down_fast[head_index]
        rates_row = token_rates[head_index]
        pre_gate = jnp.dot(gate_weight, key_fast, preferred_element_type=jnp.float32)
        pre_lift = jnp.dot(lift_weight, key_fast, preferred_element_type=jnp.float32)
        sigmoid_gate = jax.nn.sigmoid(pre_gate)
        silu_gate = pre_gate * sigmoid_gate
        hidden = (silu_gate * pre_lift).astype(jnp.bfloat16)
        target = (-(value_fast.astype(jnp.float32) * rates_row[None, :])).astype(jnp.bfloat16)
        grad_down = jnp.dot(target, hidden.T, preferred_element_type=jnp.float32)
        back_hidden = jnp.dot(down_weight.T, target, preferred_element_type=jnp.float32)
        back_lift = (back_hidden * silu_gate).astype(jnp.bfloat16)
        back_gate = (back_hidden * pre_lift * sigmoid_gate * (1.0 + pre_gate * (1.0 - sigmoid_gate))).astype(jnp.bfloat16)
        grad_gate = jnp.dot(back_gate, key_fast.T, preferred_element_type=jnp.float32)
        grad_lift = jnp.dot(back_lift, key_fast.T, preferred_element_type=jnp.float32)
        fresh_gate = refreshed(gate_weight, orthogonal(grad_gate))
        fresh_lift = refreshed(lift_weight, orthogonal(grad_lift))
        fresh_down = refreshed(down_weight, orthogonal(grad_down))
        query_gate = jnp.dot(fresh_gate, query_fast, preferred_element_type=jnp.float32)
        query_lift = jnp.dot(fresh_lift, query_fast, preferred_element_type=jnp.float32)
        query_hidden = (jax.nn.silu(query_gate) * query_lift).astype(jnp.bfloat16)
        return jnp.dot(fresh_down, query_hidden, preferred_element_type=jnp.float32).astype(jnp.bfloat16)
    recalled = lax.map(per_fast, jnp.arange(FAST_HEADS, dtype=jnp.int32)).reshape(D, TOKENS)
    return (attended, recalled)
```

```python
import functools
import math

import jax
import jax.numpy as jnp
from jax import lax
from jax.experimental import pallas as pl
from jax.experimental.pallas import tpu as pltpu
from jax.sharding import Mesh
from jax.sharding import PartitionSpec as P

WIDE = ("z", "x", "c")
EPS = 1e-06
COEF_A = 3.4445
COEF_B = -4.775
COEF_C = 2.0315
HALF = 1024
BLK = 256
NBLK = HALF // BLK
SCALE = math.log2(math.e) / math.sqrt(128)
F32 = jnp.float32
BF16 = jnp.bfloat16


def dot(a, b):
    return lax.dot_general(a, b, (((1,), (0,)), ((), ())), preferred_element_type=F32)


def dot_t(a, b):
    return lax.dot_general(a, b, (((1,), (1,)), ((), ())), preferred_element_type=F32)


def local(src, dst, sem):
    return pltpu.make_async_copy(src, dst, sem)


def remote(src, dst, send, recv, device):
    return pltpu.make_async_remote_copy(
        src_ref=src,
        dst_ref=dst,
        send_sem=send,
        recv_sem=recv,
        device_id=device,
        device_id_type=pl.DeviceIdType.MESH,
    )


def kernel(
    q_in, k_in, v_in, ck_in, cv_in, g_in, l_in, d_in, r_in,
    att, rec,
    kf, vf, kp, vp, qa, qf, wf, wd, wdt, kt, sc, ao, gd, gs, rr, yf, xs, zs, ls, fr, fd, ro, rt,
    s_loc, s_hp, s_qa, s_par, s_ring, s_fwd, s_wy, s_wp, s_wr, s_wf, s_wd, s_qf, s_rs, s_ag, s_ag2,
    s_agp, s_oa, s_or, snd,
):
    z = lax.axis_index("z")
    x = lax.axis_index("x")
    c = lax.axis_index("c")
    y = lax.axis_index("y")
    p = 1 - c
    right = lax.rem(x + 1, 4)
    left = lax.rem(x + 3, 4)
    far = lax.rem(x + 2, 4)
    onward = lax.rem(x + 1 + 2 * c, 4)
    behind = lax.rem(x + 3 + 2 * c, 4)
    me = 2 * x + c
    head = lax.rem(z, 2)
    home = z // 2
    source = y == home
    partner = (z, x, p, y)

    def rows(start, size):
        return pl.ds(pl.multiple_of(start, size), size)

    def cols(start, size):
        return pl.ds(pl.multiple_of(start, size), size)

    mine = rows(me * 64, 64)
    half = cols(c * HALF, HALF)
    other = cols(p * HALF, HALF)
    own = rows(c * 64, 64)

    loads = [
        local(k_in.at[:, half], kf.at[mine, :], s_loc.at[0]),
        local(v_in.at[:, half], vf.at[mine, :], s_loc.at[1]),
        local(q_in.at[:, cols(c * HALF + x * BLK, BLK)], qf.at[mine, :], s_loc.at[2]),
        local(r_in.at[:, cols(y * 2 * HALF + c * HALF, HALF)], rt, s_loc.at[3]),
    ]
    for load in loads:
        load.start()
    own_q = local(q_in.at[:, half], qa.at[own, :], s_qa.at[c])
    own_q.start()

    @pl.when(c == 1)
    def _():
        local(k_in.at[:, :HALF], kp.at[own, :], s_hp.at[0, c]).start()
        local(v_in.at[:, :HALF], vp.at[own, :], s_hp.at[1, c]).start()

    @pl.when((c == 0) & (y == 0))
    def _():
        local(ck_in, kp.at[own, :], s_hp.at[0, c]).start()
        local(cv_in, vp.at[own, :], s_hp.at[1, c]).start()

    full_weights = [
        local(g_in.at[head], wf.at[0], s_wy.at[0]),
        local(l_in.at[head], wf.at[1], s_wy.at[1]),
        local(d_in.at[head], wd, s_wy.at[2]),
    ]

    @pl.when(source)
    def _():
        for load in full_weights:
            load.start()

    barrier = pltpu.get_barrier_semaphore()
    peers = [partner]
    for step in range(1, 4):
        for core in range(2):
            peers.append((z, lax.rem(x + step, 4), core, y))
            peers.append((z, x, core, lax.rem(y + step, 4)))
    for peer in peers:
        pl.semaphore_signal(barrier, inc=1, device_id=peer, device_id_type=pl.DeviceIdType.MESH)
    pl.semaphore_wait(barrier, len(peers))

    gate_piece = rows(x * 128 + c * 64, 64)
    down_rows = rows(c * 256, 256)
    quarter = cols(x * 128, 128)

    @pl.when(source)
    def _():
        for step in range(1, 4):
            to = (z, x, c, lax.rem(y + step, 4))
            remote(
                g_in.at[head, gate_piece, :], wf.at[0, gate_piece, :], snd.at[0], s_wy.at[0], to
            ).start()
            remote(
                l_in.at[head, gate_piece, :], wf.at[1, gate_piece, :], snd.at[0], s_wy.at[1], to
            ).start()
            remote(
                d_in.at[head, down_rows, quarter],
                wd.at[down_rows, quarter],
                snd.at[0],
                s_wy.at[2],
                to,
            ).start()

    share = [
        remote(k_in.at[:, other], kf.at[mine, :], snd.at[1], s_par.at[0], partner),
        remote(v_in.at[:, other], vf.at[mine, :], snd.at[2], s_par.at[1], partner),
        remote(q_in.at[:, other], qa.at[own, :], snd.at[3], s_qa.at[c], partner),
    ]
    for copy in share:
        copy.start()

    def prior(ks, vs, to):
        return [
            remote(ks, kp.at[own, :], snd.at[4], s_hp.at[0, c], to),
            remote(vs, vp.at[own, :], snd.at[5], s_hp.at[1, c], to),
        ]

    within = prior(k_in.at[:, :HALF], v_in.at[:, :HALF], partner)
    cached = prior(ck_in, cv_in, partner)
    above = (z, x, 0, lax.rem(y + 1, 4))
    halo = [
        remote(k_in.at[:, HALF:], kp.at[own, :], snd.at[6], s_hp.at[0, c], above),
        remote(v_in.at[:, HALF:], vp.at[own, :], snd.at[7], s_hp.at[1, c], above),
    ]

    @pl.when(c == 0)
    def _():
        for copy in within:
            copy.start()

    @pl.when((c == 1) & (y == 0))
    def _():
        for copy in cached:
            copy.start()

    for block in range(NBLK):
        for index, (src, dst) in enumerate(((k_in, kf), (v_in, vf))):
            for way, to in enumerate((right, left)):
                for core in range(2):
                    remote(
                        src.at[:, core * HALF + block * BLK : core * HALF + (block + 1) * BLK],
                        dst.at[mine, block * BLK : (block + 1) * BLK],
                        snd.at[8 + index],
                        s_ring.at[index, block, way],
                        (z, to, core, y),
                    ).start()

    @pl.when(y < 3)
    def _():
        for copy in halo:
            copy.start()

    def ask(to_x, to_c):
        remote(
            q_in.at[:, cols(to_c * HALF + to_x * BLK, BLK)],
            qf.at[mine, :],
            snd.at[10],
            s_qf,
            (z, to_x, to_c, y),
        ).start()

    weight_share = [
        remote(wf.at[0, gate_piece, :], wf.at[0, gate_piece, :], snd.at[11], s_wp.at[0], partner),
        remote(wf.at[1, gate_piece, :], wf.at[1, gate_piece, :], snd.at[12], s_wp.at[1], partner),
        remote(
            wd.at[down_rows, quarter], wd.at[down_rows, quarter], snd.at[13], s_wp.at[2], partner
        ),
    ]
    arrivals = [
        remote(wf.at[0, gate_piece, :], wf.at[0, gate_piece, :], snd.at[11], s_wy.at[0], partner),
        remote(wf.at[1, gate_piece, :], wf.at[1, gate_piece, :], snd.at[12], s_wy.at[1], partner),
        remote(
            wd.at[down_rows, quarter], wd.at[down_rows, quarter], snd.at[13], s_wy.at[2], partner
        ),
    ]

    @pl.when(jnp.logical_not(source))
    def _():
        for copy, arrival in zip(weight_share, arrivals):
            arrival.wait_recv()
            copy.start()

    def onward_copy(index, dst, block):
        part = dst.at[rows(behind * 128, 128), block * BLK : (block + 1) * BLK]
        return remote(part, part, snd.at[14 + index], s_fwd.at[index, block], (z, onward, c, y))

    for block in range(NBLK):
        for index, dst in enumerate((kf, vf)):
            for way in range(2):
                part = dst.at[rows(behind * 128, 128), block * BLK : (block + 1) * BLK]
                remote(part, part, snd.at[14], s_ring.at[index, block, way], partner).wait_recv()
            onward_copy(index, dst, block).start()

    ask(x, p)
    for step in range(1, 4):
        for core in range(2):
            ask(lax.rem(x + step, 4), core)

    def piece_copies(chip, send, recv, to):
        gate = rows(chip * 128 + c * 64, 64)
        side = cols(chip * 128, 128)
        return [
            remote(wf.at[0, gate, :], wf.at[0, gate, :], send, recv, to),
            remote(wf.at[1, gate, :], wf.at[1, gate, :], send, recv, to),
            remote(wd.at[down_rows, side], wd.at[down_rows, side], send, recv, to),
        ]

    @pl.when(jnp.logical_not(source))
    def _():
        for way, to in enumerate((right, left)):
            for copy in piece_copies(x, snd.at[16], s_wr.at[way], (z, to, c, y)):
                copy.start()

    for load in loads:
        load.wait()
    own_q.wait()
    theirs = qa.at[rows(p * 64, 64), :]
    remote(theirs, theirs, snd.at[3], s_qa.at[p], partner).wait_recv()
    for index, dst in enumerate((kp, vp)):
        for core in range(2):
            part = dst.at[core * 64 : (core + 1) * 64, :]
            remote(part, part, snd.at[4], s_hp.at[index, core], partner).wait_recv()
    for index, dst in enumerate((kf, vf)):
        part = dst.at[rows((2 * x + p) * 64, 64), :]
        remote(part, part, snd.at[1], s_par.at[index], partner).wait_recv()

    chip = rows(x * 128, 128)
    for block in range(NBLK):
        span = slice(block * BLK, (block + 1) * BLK)
        kt[block * BLK : (block + 1) * BLK, :] = kp[:, span].T
        kt[HALF + block * BLK : HALF + (block + 1) * BLK, :] = kf[chip, span].T

    row_at = lax.broadcasted_iota(jnp.int32, (BLK, BLK), 0)
    col_at = lax.broadcasted_iota(jnp.int32, (BLK, BLK), 1)

    def attend(block):
        first = block * BLK
        asked = qa[:, first : first + BLK]
        top = jnp.full((1, BLK), -jnp.inf, F32)
        for part in range(5):
            at = first + part * BLK
            scores = dot(kt[at : at + BLK, :], asked) * SCALE
            if part == 0:
                scores = jnp.where(row_at > col_at, scores, -jnp.inf)
            if part == 4:
                scores = jnp.where(row_at <= col_at, scores, -jnp.inf)
            sc[part * BLK : (part + 1) * BLK, :] = scores
            top = jnp.maximum(top, jnp.max(scores, axis=0, keepdims=True))
        total = jnp.zeros((1, BLK), F32)
        blend = jnp.zeros((128, BLK), F32)
        for part in range(5):
            at = first + part * BLK
            raised = jnp.exp2(sc[part * BLK : (part + 1) * BLK, :] - top)
            total = total + jnp.sum(raised, axis=0, keepdims=True)
            if at < HALF:
                held = vp[:, at : at + BLK]
            else:
                held = vf[chip, at - HALF : at - HALF + BLK]
            blend = blend + dot(held, raised.astype(BF16))
        ao[:, first : first + BLK] = (blend / total).astype(BF16)

    attend(0)
    attend(1)

    @pl.when(source)
    def _():
        for load in full_weights:
            load.wait()

    @pl.when(jnp.logical_not(source))
    def _():
        theirs = rows(x * 128 + p * 64, 64)
        across = wd.at[rows(p * 256, 256), quarter]
        for index in range(2):
            part = wf.at[index, theirs, :]
            remote(part, part, snd.at[11], s_wp.at[index], partner).wait_recv()
        remote(across, across, snd.at[13], s_wp.at[2], partner).wait_recv()

    for block in range(4):
        wdt[:, block * 128 : (block + 1) * 128] = wd[block * 128 : (block + 1) * 128, quarter].T

    gd[...] = jnp.zeros_like(gd)
    for block in range(NBLK):
        span = slice(block * BLK, (block + 1) * BLK)
        for index, dst in enumerate((kf, vf)):
            part = dst.at[rows(far * 128, 128), span]
            remote(part, part, snd.at[14], s_fwd.at[index, block], partner).wait_recv()
        keys = kf[:, span]
        rate = rt[pl.ds(z, 1), span]
        target = (-(vf[:, span].astype(F32) * rate)).astype(BF16)
        pre_gate = dot(wf[0, chip, :], keys)
        pre_lift = dot(wf[1, chip, :], keys)
        back = dot(wdt[...], target)
        sig = 1.0 / (1.0 + jnp.exp(-pre_gate))
        silu = pre_gate * sig
        hidden = (silu * pre_lift).astype(BF16)
        back_lift = (back * silu).astype(BF16)
        back_gate = (back * pre_lift * sig * (1.0 + pre_gate * (1.0 - sig))).astype(BF16)
        gd[0:128, :] += dot_t(back_gate, keys)
        gd[128:256, :] += dot_t(back_lift, keys)
        gd[256:384, :] += dot_t(hidden, target)

    me_y = 2 * y + c

    for owner in range(8):
        for index in range(3):
            at = index * 128 + owner * 16
            gs[owner, index] = gd[at : at + 16, :].astype(BF16)
    for step in range(1, 8):
        owner = lax.rem(me_y + step, 8)
        remote(
            gs.at[owner], rr.at[me_y], snd.at[17], s_rs, (z, x, lax.rem(owner, 2), owner // 2)
        ).start()
    attend(2)
    remote(rr.at[0:7], rr.at[0:7], snd.at[17], s_rs, partner).wait_recv()
    place = 4 * x + y
    for index in range(3):
        whole = gd[rows(index * 128 + me_y * 16, 16), :]
        for step in range(1, 8):
            whole = whole + rr[lax.rem(me_y + step, 8), index].astype(F32)
        yf[index, place, c] = whole.astype(BF16)

    piece = yf.at[:, place, c]
    for step in range(1, 4):
        remote(piece, piece, snd.at[18], s_ag.at[0, step], (z, x, c, lax.rem(y + step, 4))).start()
        remote(piece, piece, snd.at[18], s_ag.at[1, step], (z, lax.rem(x + step, 4), c, y)).start()
    remote(piece, piece, snd.at[19], s_agp, partner).start()
    for step in range(1, 4):
        at_y = 4 * x + lax.rem(y + 4 - step, 4)
        part = yf.at[:, at_y, c]
        remote(part, part, snd.at[18], s_ag.at[0, step], partner).wait_recv()
        side = yf.at[:, at_y, c, :, 0:256]
        for hop in range(1, 4):
            remote(side, side, snd.at[20], s_ag2, (z, lax.rem(x + hop, 4), c, y)).start()
        remote(part, part, snd.at[19], s_agp, partner).start()
        at_x = 4 * lax.rem(x + 4 - step, 4) + y
        part = yf.at[:, at_x, c]
        remote(part, part, snd.at[18], s_ag.at[1, step], partner).wait_recv()
        side = yf.at[:, at_x, c, :, 256:512]
        for hop in range(1, 4):
            remote(side, side, snd.at[20], s_ag2, (z, x, c, lax.rem(y + hop, 4))).start()
        remote(part, part, snd.at[19], s_agp, partner).start()

    @pl.when(jnp.logical_not(source))
    def _():
        bytes_of = wf.at[0, 0:192, :]
        for way in range(2):
            remote(bytes_of, bytes_of, snd.at[16], s_wr.at[way], partner).wait_recv()
        for copy in piece_copies(behind, snd.at[21], s_wf, (z, onward, c, y)):
            copy.start()
        for side in (right, left):
            for copy in piece_copies(side, snd.at[22], s_wd, partner):
                copy.start()

    attend(3)
    local(ao.at[own, :], att.at[:, half], s_loc.at[4]).start()
    give = remote(ao.at[rows(p * 64, 64), :], att.at[:, half], snd.at[23], s_oa, partner)
    give.start()

    @pl.when(jnp.logical_not(source))
    def _():
        bytes_of = wf.at[0, 0:192, :]
        remote(bytes_of, bytes_of, snd.at[21], s_wf, partner).wait_recv()
        for copy in piece_copies(far, snd.at[22], s_wd, partner):
            copy.start()

    crossed = yf.at[:, 0:9, 0]
    remote(crossed, crossed, snd.at[20], s_ag2, partner).wait_recv()
    for step in range(1, 4):
        for hop in range(1, 4):
            part = yf.at[:, 4 * lax.rem(x + step, 4) + lax.rem(y + hop, 4), c]
            remote(part, part, snd.at[19], s_agp, partner).start()
    remote(yf.at[:, :, 0], yf.at[:, :, 0], snd.at[19], s_agp, partner).wait_recv()

    def ortho(index, carry):
        rounded = yf[index].reshape(512, 512).astype(F32)
        norm = jnp.sqrt(jnp.sum(jnp.square(rounded), keepdims=True) + EPS)
        xs[index] = (rounded / norm).astype(BF16)
        for _ in range(2):
            zs[...] = dot_t(xs[index], xs[index]).astype(BF16)
            ls[...] = dot(zs[...], xs[index]).astype(BF16)
            xs[index] = (
                COEF_A * xs[index].astype(F32)
                + COEF_B * ls[...].astype(F32)
                + COEF_C * dot(zs[...], ls[...])
            ).astype(BF16)
        return carry

    lax.fori_loop(0, 3, ortho, 0)

    @pl.when(jnp.logical_not(source))
    def _():
        bytes_of = kf.at[0:288, :]
        remote(bytes_of, bytes_of, snd.at[22], s_wd, partner).wait_recv()

    def fresh(weight, turned):
        initial = weight.astype(F32)
        moved = initial - turned.astype(F32)
        wanted = jnp.sqrt(jnp.mean(jnp.square(initial), axis=-1, keepdims=True) + EPS)
        present = jnp.sqrt(jnp.mean(jnp.square(moved), axis=-1, keepdims=True) + EPS)
        return (moved * (wanted / present)).astype(BF16)

    for index in range(2):
        fr[index] = fresh(wf[index], xs[index])
    fd[...] = fresh(wd[...], xs[2].T)

    remote(qf.at[0:448, :], qf.at[0:448, :], snd.at[10], s_qf, partner).wait_recv()
    query_gate = dot(fr[0], qf[...])
    query_lift = dot(fr[1], qf[...])
    query_hidden = (query_gate / (1.0 + jnp.exp(-query_gate)) * query_lift).astype(BF16)
    ro[...] = dot(fd[...], query_hidden).astype(BF16)
    tokens = cols(c * HALF + x * BLK, BLK)

    def answer(to_x, to_c):
        remote(
            ro.at[rows((2 * to_x + to_c) * 64, 64), :],
            rec.at[:, tokens],
            snd.at[24],
            s_or,
            (z, to_x, to_c, y),
        ).start()

    for step in (2, 1, 3):
        for core in range(2):
            answer(lax.rem(x + step, 4), core)
    answer(x, p)
    local(ro.at[mine, :], rec.at[:, tokens], s_loc.at[5]).start()

    local(ao.at[own, :], att.at[:, half], s_loc.at[4]).wait()
    local(ro.at[mine, :], rec.at[:, tokens], s_loc.at[5]).wait()
    give.wait_send()
    remote(ao.at[own, :], att.at[:, other], snd.at[23], s_oa, partner).wait_recv()
    for copy in share:
        copy.wait_send()

    @pl.when(c == 0)
    def _():
        for copy in within:
            copy.wait_send()

    @pl.when((c == 1) & (y == 0))
    def _():
        for copy in cached:
            copy.wait_send()

    @pl.when(y < 3)
    def _():
        for copy in halo:
            copy.wait_send()

    def drain(ref, index):
        remote(ref, ref, snd.at[index], s_or, partner).wait_send()

    @pl.when(source)
    def _():
        drain(kf.at[0:288, :], 0)

    for index in range(2):
        drain(kf.at[0:256, :], 8 + index)
        drain(kf.at[0:128, :], 14 + index)
    drain(qf.at[0:448, :], 10)

    @pl.when(jnp.logical_not(source))
    def _():
        for copy in weight_share:
            copy.wait_send()
        drain(wf.at[0, 0:384, :], 16)
        drain(wf.at[0, 0:192, :], 21)
        drain(kf.at[0:288, :], 22)

    drain(rr.at[0:7], 17)
    drain(yf.at[:, 0:6, 0], 18)
    drain(yf.at[:, :, 0], 19)
    drain(yf.at[:, 0:9, 0], 20)
    drain(qf.at[0:448, :], 24)
    remote(qf.at[0:448, :], qf.at[0:448, :], snd.at[24], s_or, partner).wait_recv()


def per_device(*arrays):
    any_spec = pl.BlockSpec(memory_space=pl.ANY)
    out = jax.ShapeDtypeStruct((64, 2 * HALF), BF16)
    vmem = pltpu.VMEM
    dma = pltpu.SemaphoreType.DMA
    return pl.pallas_call(
        kernel,
        out_shape=(out, out),
        in_specs=[any_spec] * 9,
        out_specs=(any_spec, any_spec),
        scratch_shapes=[
            vmem((512, HALF), BF16),
            vmem((512, HALF), BF16),
            vmem((128, HALF), BF16),
            vmem((128, HALF), BF16),
            vmem((128, HALF), BF16),
            vmem((512, BLK), BF16),
            vmem((2, 512, 512), BF16),
            vmem((512, 512), BF16),
            vmem((128, 512), BF16),
            vmem((2 * HALF, 128), BF16),
            vmem((5 * BLK, BLK), F32),
            vmem((128, HALF), BF16),
            vmem((384, 512), F32),
            vmem((8, 3, 16, 512), BF16),
            vmem((8, 3, 16, 512), BF16),
            vmem((3, 16, 2, 16, 512), BF16),
            vmem((3, 512, 512), BF16),
            vmem((512, 512), BF16),
            vmem((512, 512), BF16),
            vmem((2, 512, 512), BF16),
            vmem((512, 512), BF16),
            vmem((512, BLK), BF16),
            vmem((8, HALF), F32),
            dma((6,)),
            dma((2, 2)),
            dma((2,)),
            dma((2,)),
            dma((2, NBLK, 2)),
            dma((2, NBLK)),
            dma((3,)),
            dma((3,)),
            dma((2,)),
            dma(()),
            dma(()),
            dma(()),
            dma(()),
            dma((2, 4)),
            dma(()),
            dma(()),
            dma(()),
            dma(()),
            dma((25,)),
        ],
        compiler_params=pltpu.CompilerParams(
            collective_id=0, has_side_effects=True, vmem_limit_bytes=48 * 1024 * 1024
        ),
        name="plane",
    )(*arrays)


def solution(mesh):
    split = Mesh(mesh.devices.reshape(8, 4, 2, 4), ("z", "x", "c", "y"))
    tokens = P(WIDE, "y")
    heads = P("y", None, None)
    return jax.shard_map(
        per_device,
        mesh=split,
        in_specs=(tokens, tokens, tokens, P(WIDE), P(WIDE), heads, heads, heads, P()),
        out_specs=(tokens, tokens),
        check_vma=False,
    )
```

```python
import functools
import math

import jax
import jax.numpy as jnp
from jax import lax
from jax.experimental import pallas as pl
from jax.experimental.pallas import tpu as pltpu
from jax.sharding import Mesh
from jax.sharding import PartitionSpec as P

WIDE = ("z", "x", "c")
EPS = 1e-06
COEF_A = 3.4445
COEF_B = -4.775
COEF_C = 2.0315
HALF = 1024
BLK = 256
NBLK = HALF // BLK
SCALE = math.log2(math.e) / math.sqrt(128)
F32 = jnp.float32
BF16 = jnp.bfloat16


def dot(a, b):
    return lax.dot_general(a, b, (((1,), (0,)), ((), ())), preferred_element_type=F32)


def dot_t(a, b):
    return lax.dot_general(a, b, (((1,), (1,)), ((), ())), preferred_element_type=F32)


def local(src, dst, sem):
    return pltpu.make_async_copy(src, dst, sem)


def remote(src, dst, send, recv, device):
    return pltpu.make_async_remote_copy(
        src_ref=src,
        dst_ref=dst,
        send_sem=send,
        recv_sem=recv,
        device_id=device,
        device_id_type=pl.DeviceIdType.MESH,
    )


def kernel(
    q_in, k_in, v_in, ck_in, cv_in, g_in, l_in, d_in, r_in,
    att, rec,
    kf, vf, qf, kp, vp, wm, wq, wdq, wdr, wdt, kt, sc, ao, gd, ps, pr, gs, rr, ym, yd, xs, zs, ls,
    fr, fd, ro, rt,
    s_loc, s_hp, s_par, s_ring, s_fwd, s_wy, s_wp, s_wr, s_wf, s_qr, s_qfw, s_rsp, s_rs, s_ag, s_ag2,
    s_dag, s_dag2, s_dp, s_fr, s_oa, s_or, snd,
):
    z = lax.axis_index("z")
    x = lax.axis_index("x")
    c = lax.axis_index("c")
    y = lax.axis_index("y")
    p = 1 - c
    right = lax.rem(x + 1, 4)
    left = lax.rem(x + 3, 4)
    far = lax.rem(x + 2, 4)
    onward = lax.rem(x + 1 + 2 * c, 4)
    behind = lax.rem(x + 3 + 2 * c, 4)
    me = 2 * x + c
    head = lax.rem(z, 2)
    source = y == z // 2
    partner = (z, x, p, y)

    def at(start, size):
        return pl.ds(pl.multiple_of(start, size), size)

    mine = at(me * 64, 64)
    half = at(c * HALF, HALF)
    other = at(p * HALF, HALF)
    own = at(c * 64, 64)
    theirs = at(p * 64, 64)
    quarter = at(x * 128, 128)
    down_rows = at(c * 256, 256)
    down_piece = at(x * 128 + c * 64, 64)

    def got(ref, sem):
        remote(ref, ref, snd.at[0], sem, partner).wait_recv()

    loads = [
        local(k_in.at[:, half], kf.at[mine, :], s_loc.at[0]),
        local(v_in.at[:, half], vf.at[mine, :], s_loc.at[1]),
        local(q_in.at[:, half], qf.at[mine, :], s_loc.at[2]),
        local(r_in.at[:, at(y * 2 * HALF + c * HALF, HALF)], rt, s_loc.at[3]),
    ]
    for load in loads:
        load.start()

    @pl.when(c == 1)
    def _():
        local(k_in.at[:, :HALF], kp.at[own, :], s_hp.at[0, c]).start()
        local(v_in.at[:, :HALF], vp.at[own, :], s_hp.at[1, c]).start()

    @pl.when((c == 0) & (y == 0))
    def _():
        local(ck_in, kp.at[own, :], s_hp.at[0, c]).start()
        local(cv_in, vp.at[own, :], s_hp.at[1, c]).start()

    def full_weights(first, second):
        return [
            local(first.at[head], wm, s_wy.at[0]),
            local(second.at[head, quarter, :], wq.at[at(p * 128, 128), :], s_wy.at[1]),
            local(d_in.at[head, :, quarter], wdq, s_wy.at[2]),
            local(d_in.at[head, quarter, :], wdr, s_wy.at[3]),
        ]

    for core, (first, second) in enumerate(((g_in, l_in), (l_in, g_in))):

        @pl.when(source & (c == core))
        def _():
            for load in full_weights(first, second):
                load.start()

    barrier = pltpu.get_barrier_semaphore()
    peers = [partner]
    for step in range(1, 4):
        for core in range(2):
            peers.append((z, lax.rem(x + step, 4), core, y))
            peers.append((z, x, core, lax.rem(y + step, 4)))
    for peer in peers:
        pl.semaphore_signal(barrier, inc=1, device_id=peer, device_id_type=pl.DeviceIdType.MESH)
    pl.semaphore_wait(barrier, len(peers))

    for core, first in enumerate((g_in, l_in)):

        @pl.when(source & (c == core))
        def _():
            for step in (2, 1, 3):
                to = (z, x, c, lax.rem(y + step, 4))
                remote(
                    first.at[head, quarter, :], wm.at[quarter, :], snd.at[0], s_wy.at[0], to
                ).start()
                remote(
                    d_in.at[head, down_rows, quarter],
                    wdq.at[down_rows, :],
                    snd.at[0],
                    s_wy.at[1],
                    to,
                ).start()

    share = [
        remote(k_in.at[:, other], kf.at[mine, :], snd.at[1], s_par.at[0], partner),
        remote(v_in.at[:, other], vf.at[mine, :], snd.at[2], s_par.at[1], partner),
        remote(q_in.at[:, other], qf.at[mine, :], snd.at[3], s_par.at[2], partner),
    ]
    for copy in share:
        copy.start()

    def prior(ks, vs, to, index):
        return [
            remote(ks, kp.at[own, :], snd.at[index], s_hp.at[0, c], to),
            remote(vs, vp.at[own, :], snd.at[index + 1], s_hp.at[1, c], to),
        ]

    within = prior(k_in.at[:, :HALF], v_in.at[:, :HALF], partner, 4)
    cached = prior(ck_in, cv_in, partner, 4)
    halo = prior(k_in.at[:, HALF:], v_in.at[:, HALF:], (z, x, 0, lax.rem(y + 1, 4)), 25)

    @pl.when(c == 0)
    def _():
        for copy in within:
            copy.start()

    @pl.when((c == 1) & (y == 0))
    def _():
        for copy in cached:
            copy.start()

    def spread(src, dst, send, recv, first, size):
        for way, to in enumerate((right, left)):
            for core in range(2):
                remote(
                    src.at[:, core * HALF + first : core * HALF + first + size],
                    dst.at[mine, first : first + size],
                    send,
                    recv.at[way],
                    (z, to, core, y),
                ).start()

    for block in range(NBLK):
        for index, (src, dst) in enumerate(((k_in, kf), (v_in, vf))):
            spread(src, dst, snd.at[8 + index], s_ring.at[index, block], block * BLK, BLK)

    @pl.when(y < 3)
    def _():
        for copy in halo:
            copy.start()

    @pl.when(source)
    def _():
        for step in (2, 1, 3):
            to = (z, x, c, lax.rem(y + step, 4))
            remote(
                d_in.at[head, down_piece, :], wdr.at[own, :], snd.at[6], s_wy.at[2], to
            ).start()

    for block in range(NBLK):
        span = slice(block * BLK, (block + 1) * BLK)
        for index, dst in enumerate((kf, vf)):
            part = dst.at[at(behind * 128, 128), span]
            for way in range(2):
                got(part, s_ring.at[index, block, way])
            remote(part, part, snd.at[14], s_fwd.at[index, block], (z, onward, c, y)).start()

    spread(q_in, qf, snd.at[10], s_qr, 0, HALF)

    wm_quarter = wm.at[quarter, :]
    weight_share = [
        remote(wm_quarter, wq.at[at(c * 128, 128), :], snd.at[11], s_wp.at[0], partner),
        remote(wdq.at[down_rows, :], wdq.at[down_rows, :], snd.at[12], s_wp.at[1], partner),
    ]

    @pl.when(jnp.logical_not(source))
    def _():
        got(wm_quarter, s_wy.at[0])
        got(wdq.at[down_rows, :], s_wy.at[1])
        for copy in weight_share:
            copy.start()
        for way, to in enumerate((right, left)):
            remote(wm_quarter, wm_quarter, snd.at[16], s_wr.at[way], (z, to, c, y)).start()

    for load in loads:
        load.wait()
    for index, dst in enumerate((kp, vp)):
        for core in range(2):
            got(dst.at[core * 64 : (core + 1) * 64, :], s_hp.at[index, core])
    for index, dst in enumerate((kf, vf, qf)):
        got(dst.at[at((2 * x + p) * 64, 64), :], s_par.at[index])

    for block in range(NBLK):
        span = slice(block * BLK, (block + 1) * BLK)
        kt[block * BLK : (block + 1) * BLK, :] = kp[:, span].T
        kt[HALF + block * BLK : HALF + (block + 1) * BLK, :] = kf[quarter, span].T

    row_at = lax.broadcasted_iota(jnp.int32, (BLK, BLK), 0)
    col_at = lax.broadcasted_iota(jnp.int32, (BLK, BLK), 1)

    def attend(block):
        first = block * BLK
        asked = qf[quarter, first : first + BLK]
        top = jnp.full((1, BLK), -jnp.inf, F32)
        for part in range(5):
            key = first + part * BLK
            scores = dot(kt[key : key + BLK, :], asked) * SCALE
            if part == 0:
                scores = jnp.where(row_at > col_at, scores, -jnp.inf)
            if part == 4:
                scores = jnp.where(row_at <= col_at, scores, -jnp.inf)
            sc[part * BLK : (part + 1) * BLK, :] = scores
            top = jnp.maximum(top, jnp.max(scores, axis=0, keepdims=True))
        total = jnp.zeros((1, BLK), F32)
        blend = jnp.zeros((128, BLK), F32)
        for part in range(5):
            key = first + part * BLK
            raised = jnp.exp2(sc[part * BLK : (part + 1) * BLK, :] - top)
            total = total + jnp.sum(raised, axis=0, keepdims=True)
            if key < HALF:
                held = vp[:, key : key + BLK]
            else:
                held = vf[quarter, key - HALF : key - HALF + BLK]
            blend = blend + dot(held, raised.astype(BF16))
        ao[:, first : first + BLK] = (blend / total).astype(BF16)

    attend(0)

    for core, (first, second) in enumerate(((g_in, l_in), (l_in, g_in))):

        @pl.when(source & (c == core))
        def _():
            for load in full_weights(first, second):
                load.wait()

    @pl.when(jnp.logical_not(source))
    def _():
        got(wq.at[at(p * 128, 128), :], s_wp.at[0])
        got(wdq.at[at(p * 256, 256), :], s_wp.at[1])

    wq[at(c * 128, 128), :] = wm[quarter, :]
    for block in range(4):
        wdt[:, block * 128 : (block + 1) * 128] = wdq[block * 128 : (block + 1) * 128, :].T

    gd[...] = jnp.zeros_like(gd)
    for block in range(NBLK):
        span = slice(block * BLK, (block + 1) * BLK)
        for index, dst in enumerate((kf, vf)):
            got(dst.at[at(far * 128, 128), span], s_fwd.at[index, block])
        keys = kf[:, span]
        rate = rt[pl.ds(z, 1), span]
        target = (-(vf[:, span].astype(F32) * rate)).astype(BF16)
        pre_gate = dot(wq[0:128, :], keys)
        pre_lift = dot(wq[128:256, :], keys)
        back = dot(wdt[...], target)
        sig = 1.0 / (1.0 + jnp.exp(-pre_gate))
        silu = pre_gate * sig
        hidden = (silu * pre_lift).astype(BF16)
        back_lift = (back * silu).astype(BF16)
        back_gate = (back * pre_lift * sig * (1.0 + pre_gate * (1.0 - sig))).astype(BF16)
        gd[0:128, :] += dot_t(back_gate, keys)
        gd[128:256, :] += dot_t(back_lift, keys)
        gd[256:384, :] += dot_t(hidden, target)

    ps[0:128, :] = gd[at(p * 128, 128), :].astype(BF16)
    ps[128:192, :] = gd[at(256 + p * 64, 64), :].astype(BF16)
    remote(ps, pr, snd.at[15], s_rsp, partner).start()
    attend(1)
    got(pr, s_rsp)
    for owner in range(4):
        main = gd[at(c * 128 + owner * 32, 32), :] + pr[owner * 32 : owner * 32 + 32, :].astype(F32)
        down = (
            gd[at(256 + c * 64 + owner * 16, 16), :]
            + pr[128 + owner * 16 : 144 + owner * 16, :].astype(F32)
        )
        gs[owner, 0:32, :] = main.astype(BF16)
        gs[owner, 32:48, :] = down.astype(BF16)
        ls[owner * 48 : owner * 48 + 32, :] = main
        ls[owner * 48 + 32 : owner * 48 + 48, :] = down
    for step in (2, 1, 3):
        owner = lax.rem(y + step, 4)
        remote(gs.at[owner], rr.at[y], snd.at[17], s_rs, (z, x, c, owner)).start()
    attend(2)
    attend(3)
    local(ao.at[own, :], att.at[:, half], s_loc.at[4]).start()
    give = remote(ao.at[theirs, :], att.at[:, half], snd.at[23], s_oa, partner)
    give.start()
    got(rr.at[0:3], s_rs)
    whole = ls[at(y * 48, 48), :]
    for step in range(1, 4):
        whole = whole + rr[lax.rem(y + step, 4)].astype(F32)
    place = 4 * x + y
    ym[place] = whole[0:32].astype(BF16)
    mark_d = 4 * (2 * x + c) + y
    yd[mark_d] = whole[32:48].astype(BF16)

    def gather(ref, index_of, first, second, send):
        own_piece = index_of(x, y)
        low, high = slice(0, 256), slice(256, 512)

        def put(index, span, recv, to):
            part = ref.at[index, :, span]
            remote(part, part, send, recv, to).start()

        for step in (2, 1, 3):
            put(own_piece, low, first.at[0, step], (z, x, c, lax.rem(y + step, 4)))
            put(own_piece, high, first.at[1, step], (z, lax.rem(x + step, 4), c, y))
        for step in (2, 1, 3):
            put(own_piece, low, second, (z, lax.rem(x + step, 4), c, y))
            put(own_piece, high, second, (z, x, c, lax.rem(y + step, 4)))

    def relay(ref, index_of, first, second, send):
        low, high = slice(0, 256), slice(256, 512)
        for step in (1, 3, 2):
            across = index_of(x, lax.rem(y + 4 - step, 4))
            part = ref.at[across, :, low]
            got(part, first.at[0, step])
            for hop in (2, 1, 3):
                to = (z, lax.rem(x + hop, 4), c, y)
                remote(part, part, send, second, to).start()
            along = index_of(lax.rem(x + 4 - step, 4), y)
            part = ref.at[along, :, high]
            got(part, first.at[1, step])
            for hop in (2, 1, 3):
                to = (z, x, c, lax.rem(y + hop, 4))
                remote(part, part, send, second, to).start()

    def main_at(xx, yy):
        return 4 * xx + yy

    def down_at(xx, yy):
        return 4 * (2 * xx + c) + yy

    gather(ym, main_at, s_ag, s_ag2, snd.at[18])
    gather(yd, down_at, s_dag, s_dag2, snd.at[19])
    relay(ym, main_at, s_ag, s_ag2, snd.at[18])
    relay(yd, down_at, s_dag, s_dag2, snd.at[19])

    @pl.when(jnp.logical_not(source))
    def _():
        for way in range(2):
            got(wm_quarter, s_wr.at[way])
        part = wm.at[at(behind * 128, 128), :]
        remote(part, part, snd.at[21], s_wf, (z, onward, c, y)).start()
        got(wdr.at[own, :], s_wy.at[2])
        remote(wdr.at[own, :], wdr.at[own, :], snd.at[22], s_wp.at[2], partner).start()

    for way in range(2):
        got(qf.at[at(behind * 128, 128), :], s_qr.at[way])
    part = qf.at[at(behind * 128, 128), :]
    remote(part, part, snd.at[7], s_qfw, (z, onward, c, y)).start()

    def begin(rounded):
        wide = rounded.astype(F32)
        norm = jnp.sqrt(jnp.sum(jnp.square(wide), keepdims=True) + EPS)
        return (wide / norm).astype(BF16)

    def sweep():
        zs[...] = dot_t(xs[...], xs[...]).astype(BF16)
        fd[...] = dot(zs[...], xs[...]).astype(BF16)
        xs[...] = (
            COEF_A * xs[...].astype(F32)
            + COEF_B * fd[...].astype(F32)
            + COEF_C * dot(zs[...], fd[...])
        ).astype(BF16)

    def fresh(weight, turned):
        initial = weight.astype(F32)
        moved = initial - turned.astype(F32)
        wanted = jnp.sqrt(jnp.mean(jnp.square(initial), axis=-1, keepdims=True) + EPS)
        present = jnp.sqrt(jnp.mean(jnp.square(moved), axis=-1, keepdims=True) + EPS)
        return (moved * (wanted / present)).astype(BF16)

    got(ym.at[0:12], s_ag2)
    xs[...] = begin(ym[...].reshape(512, 512))
    sweep()
    sweep()

    got(yd.at[0:12], s_dag2)
    halves = [yd.at[at(8 * chip + 4 * c, 4)] for chip in range(4)]
    for chip in range(4):
        remote(halves[chip], halves[chip], snd.at[20], s_dp, partner).start()

    @pl.when(jnp.logical_not(source))
    def _():
        got(wm.at[at(far * 128, 128), :], s_wf)

    fr[c] = fresh(wm[...], xs[...])
    lend = remote(fr.at[c], fr.at[c], snd.at[13], s_fr, partner)
    lend.start()

    got(yd.at[0:16], s_dp)
    xs[...] = begin(yd[...].reshape(512, 512))
    sweep()
    zs[...] = dot_t(xs[...], xs[...]).astype(BF16)
    side = xs[:, quarter]
    lifted = dot(zs[...], side).astype(BF16)
    turned = (
        COEF_A * side.astype(F32) + COEF_B * lifted.astype(F32) + COEF_C * dot(zs[...], lifted)
    ).astype(BF16)

    @pl.when(jnp.logical_not(source))
    def _():
        got(wdr.at[theirs, :], s_wp.at[2])

    wdt[...] = fresh(wdr[...], turned.T)

    got(qf.at[at(far * 128, 128), :], s_qfw)
    got(fr.at[p], s_fr)
    for block in range(NBLK):
        span = slice(block * BLK, (block + 1) * BLK)
        asked = qf[:, span]
        query_gate = dot(fr[0], asked)
        query_lift = dot(fr[1], asked)
        query_hidden = (query_gate / (1.0 + jnp.exp(-query_gate)) * query_lift).astype(BF16)
        ro[:, span] = dot(wdt[...], query_hidden).astype(BF16)
        here = at(c * HALF + block * BLK, BLK)
        remote(ro.at[theirs, span], rec.at[:, here], snd.at[24], s_or, partner).start()
        local(ro.at[own, span], rec.at[:, here], s_loc.at[5 + block]).start()

    def drain(ref, index):
        remote(ref, ref, snd.at[index], s_or, partner).wait_send()

    for block in range(NBLK):
        span = slice(block * BLK, (block + 1) * BLK)
        local(ro.at[own, span], ro.at[own, span], s_loc.at[5 + block]).wait()
    local(ao.at[own, :], att.at[:, half], s_loc.at[4]).wait()
    give.wait_send()
    got(ao.at[own, :], s_oa)
    lend.wait_send()
    for copy in share:
        copy.wait_send()

    @pl.when(c == 0)
    def _():
        for copy in within:
            copy.wait_send()

    @pl.when((c == 1) & (y == 0))
    def _():
        for copy in cached:
            copy.wait_send()

    @pl.when(y < 3)
    def _():
        for copy in halo:
            copy.wait_send()

    @pl.when(source)
    def _():
        drain(kf.at[0:288, :], 0)
        drain(wm.at[0:192, :], 6)

    for index in range(2):
        drain(kf.at[0:256, :], 8 + index)
    drain(kf.at[0:256, :], 14)
    drain(kf.at[0:256, :], 10)
    drain(kf.at[0:128, :], 7)

    @pl.when(jnp.logical_not(source))
    def _():
        for copy in weight_share:
            copy.wait_send()
        drain(wm.at[0:256, :], 16)
        drain(wm.at[0:128, :], 21)
        drain(wdr.at[own, :], 22)

    drain(pr, 15)
    drain(rr.at[0:3], 17)
    drain(ym.at[0:15], 18)
    drain(yd.at[0:15], 19)
    drain(yd.at[0:16], 20)
    drain(ro.at[0:64, :], 24)
    got(ro.at[0:64, :], s_or)


def per_device(*arrays):
    any_spec = pl.BlockSpec(memory_space=pl.ANY)
    out = jax.ShapeDtypeStruct((64, 2 * HALF), BF16)
    vmem = pltpu.VMEM
    dma = pltpu.SemaphoreType.DMA
    return pl.pallas_call(
        kernel,
        out_shape=(out, out),
        in_specs=[any_spec] * 9,
        out_specs=(any_spec, any_spec),
        scratch_shapes=[
            vmem((512, HALF), BF16),
            vmem((512, HALF), BF16),
            vmem((512, HALF), BF16),
            vmem((128, HALF), BF16),
            vmem((128, HALF), BF16),
            vmem((512, 512), BF16),
            vmem((256, 512), BF16),
            vmem((512, 128), BF16),
            vmem((128, 512), BF16),
            vmem((128, 512), BF16),
            vmem((2 * HALF, 128), BF16),
            vmem((5 * BLK, BLK), F32),
            vmem((128, HALF), BF16),
            vmem((384, 512), F32),
            vmem((192, 512), BF16),
            vmem((192, 512), BF16),
            vmem((4, 48, 512), BF16),
            vmem((4, 48, 512), BF16),
            vmem((16, 32, 512), BF16),
            vmem((32, 16, 512), BF16),
            vmem((512, 512), BF16),
            vmem((512, 512), BF16),
            vmem((192, 512), F32),
            vmem((2, 512, 512), BF16),
            vmem((512, 512), BF16),
            vmem((128, HALF), BF16),
            vmem((8, HALF), F32),
            dma((9,)),
            dma((2, 2)),
            dma((3,)),
            dma((2, NBLK, 2)),
            dma((2, NBLK)),
            dma((4,)),
            dma((3,)),
            dma((2,)),
            dma(()),
            dma((2,)),
            dma(()),
            dma(()),
            dma(()),
            dma((2, 4)),
            dma(()),
            dma((2, 4)),
            dma(()),
            dma(()),
            dma(()),
            dma(()),
            dma(()),
            dma((27,)),
        ],
        compiler_params=pltpu.CompilerParams(
            collective_id=0, has_side_effects=True, vmem_limit_bytes=67000000
        ),
        name="plane",
    )(*arrays)


def solution(mesh):
    split = Mesh(mesh.devices.reshape(8, 4, 2, 4), ("z", "x", "c", "y"))
    tokens = P(WIDE, "y")
    heads = P("y", None, None)
    return jax.shard_map(
        per_device,
        mesh=split,
        in_specs=(tokens, tokens, tokens, P(WIDE), P(WIDE), heads, heads, heads, P()),
        out_specs=(tokens, tokens),
        check_vma=False,
    )
```

```python
import functools
import math

import jax
import jax.numpy as jnp
from jax import lax
from jax.experimental import pallas as pl
from jax.experimental.pallas import tpu as pltpu
from jax.sharding import Mesh
from jax.sharding import PartitionSpec as P

WIDE = ("z", "x", "c")
EPS = 1e-06
COEF_A = 3.4445
COEF_B = -4.775
COEF_C = 2.0315
HALF = 1024
BLK = 256
NBLK = HALF // BLK
SCALE = math.log2(math.e) / math.sqrt(128)
F32 = jnp.float32
BF16 = jnp.bfloat16


def dot(a, b):
    return lax.dot_general(a, b, (((1,), (0,)), ((), ())), preferred_element_type=F32)


def dot_t(a, b):
    return lax.dot_general(a, b, (((1,), (1,)), ((), ())), preferred_element_type=F32)


def local(src, dst, sem):
    return pltpu.make_async_copy(src, dst, sem)


def remote(src, dst, send, recv, device):
    return pltpu.make_async_remote_copy(
        src_ref=src,
        dst_ref=dst,
        send_sem=send,
        recv_sem=recv,
        device_id=device,
        device_id_type=pl.DeviceIdType.MESH,
    )


def kernel(
    q_in, k_in, v_in, ck_in, cv_in, g_in, l_in, d_in, r_in,
    att, rec,
    kf, vf, qf, kp, vp, wm, wq, wdq, wdr, wdt, kt, sc, ao, gd, ps, pr, gs, rr, ym, yd, xs, zs, ls,
    fr, fd, ro, rt,
    s_loc, s_hp, s_par, s_ring, s_fwd, s_wy, s_wp, s_wr, s_wf, s_qr, s_qfw, s_rsp, s_rs, s_ag, s_ag2,
    s_dag, s_dag2, s_dp, s_fr, s_oa, s_or, snd,
):
    z = lax.axis_index("z")
    x = lax.axis_index("x")
    c = lax.axis_index("c")
    y = lax.axis_index("y")
    p = 1 - c
    right = lax.rem(x + 1, 4)
    left = lax.rem(x + 3, 4)
    far = lax.rem(x + 2, 4)
    me = 2 * x + c
    head = lax.rem(z, 2)
    source = y == z // 2
    partner = (z, x, p, y)

    def at(start, size):
        return pl.ds(pl.multiple_of(start, size), size)

    mine = at(me * 64, 64)
    half = at(c * HALF, HALF)
    other = at(p * HALF, HALF)
    own = at(c * 64, 64)
    theirs = at(p * 64, 64)
    quarter = at(x * 128, 128)
    down_rows = at(c * 256, 256)
    down_piece = at(x * 128 + c * 64, 64)

    def got(ref, sem):
        remote(ref, ref, snd.at[0], sem, partner).wait_recv()

    loads = [
        local(k_in.at[:, half], kf.at[mine, :], s_loc.at[0]),
        local(v_in.at[:, half], vf.at[mine, :], s_loc.at[1]),
        local(q_in.at[:, half], qf.at[mine, :], s_loc.at[2]),
        local(r_in.at[:, at(y * 2 * HALF + c * HALF, HALF)], rt, s_loc.at[3]),
    ]
    for load in loads:
        load.start()

    @pl.when(c == 1)
    def _():
        local(k_in.at[:, :HALF], kp.at[own, :], s_hp.at[0, c]).start()
        local(v_in.at[:, :HALF], vp.at[own, :], s_hp.at[1, c]).start()

    @pl.when((c == 0) & (y == 0))
    def _():
        local(ck_in, kp.at[own, :], s_hp.at[0, c]).start()
        local(cv_in, vp.at[own, :], s_hp.at[1, c]).start()

    def full_weights(first, second):
        return [
            local(first.at[head], wm, s_wy.at[0]),
            local(second.at[head, quarter, :], wq.at[at(p * 128, 128), :], s_wy.at[1]),
            local(d_in.at[head, :, quarter], wdq, s_wy.at[2]),
            local(d_in.at[head, quarter, :], wdr, s_wy.at[3]),
        ]

    for core, (first, second) in enumerate(((g_in, l_in), (l_in, g_in))):

        @pl.when(source & (c == core))
        def _():
            for load in full_weights(first, second):
                load.start()

    barrier = pltpu.get_barrier_semaphore()
    peers = [partner]
    for step in range(1, 4):
        for core in range(2):
            peers.append((z, lax.rem(x + step, 4), core, y))
            peers.append((z, x, core, lax.rem(y + step, 4)))
    for peer in peers:
        pl.semaphore_signal(barrier, inc=1, device_id=peer, device_id_type=pl.DeviceIdType.MESH)
    pl.semaphore_wait(barrier, len(peers))

    for core, first in enumerate((g_in, l_in)):

        @pl.when(source & (c == core))
        def _():
            for step in (2, 1, 3):
                to = (z, x, c, lax.rem(y + step, 4))
                remote(
                    first.at[head, quarter, :], wm.at[quarter, :], snd.at[0], s_wy.at[0], to
                ).start()
                remote(
                    d_in.at[head, down_rows, quarter],
                    wdq.at[down_rows, :],
                    snd.at[0],
                    s_wy.at[1],
                    to,
                ).start()

    share = [
        remote(k_in.at[:, other], kf.at[mine, :], snd.at[1], s_par.at[0], partner),
        remote(v_in.at[:, other], vf.at[mine, :], snd.at[2], s_par.at[1], partner),
        remote(q_in.at[:, other], qf.at[mine, :], snd.at[3], s_par.at[2], partner),
    ]
    for copy in share:
        copy.start()

    def prior(ks, vs, to, index):
        return [
            remote(ks, kp.at[own, :], snd.at[index], s_hp.at[0, c], to),
            remote(vs, vp.at[own, :], snd.at[index + 1], s_hp.at[1, c], to),
        ]

    within = prior(k_in.at[:, :HALF], v_in.at[:, :HALF], partner, 4)
    cached = prior(ck_in, cv_in, partner, 4)
    halo = prior(k_in.at[:, HALF:], v_in.at[:, HALF:], (z, x, 0, lax.rem(y + 1, 4)), 25)

    @pl.when(c == 0)
    def _():
        for copy in within:
            copy.start()

    @pl.when((c == 1) & (y == 0))
    def _():
        for copy in cached:
            copy.start()

    def spread(src, dst, send, recv, first, size):
        for way, to in enumerate((right, left)):
            for core in range(2):
                remote(
                    src.at[:, core * HALF + first : core * HALF + first + size],
                    dst.at[mine, first : first + size],
                    send,
                    recv.at[way],
                    (z, to, core, y),
                ).start()

    for block in range(NBLK):
        for index, (src, dst) in enumerate(((k_in, kf), (v_in, vf))):
            spread(src, dst, snd.at[8 + index], s_ring.at[index, block], block * BLK, BLK)

    @pl.when(y < 3)
    def _():
        for copy in halo:
            copy.start()

    @pl.when(source)
    def _():
        for step in (2, 1, 3):
            to = (z, x, c, lax.rem(y + step, 4))
            remote(
                d_in.at[head, down_piece, :], wdr.at[own, :], snd.at[6], s_wy.at[2], to
            ).start()

    chips = (left, right)
    for block in range(NBLK):
        span = slice(block * BLK, (block + 1) * BLK)
        for index, dst in enumerate((kf, vf)):
            part = dst.at[at(chips[index] * 128, 128), span]
            got(part, s_ring.at[index, block, index])
            to = (z, chips[1 - index], c, y)
            remote(part, part, snd.at[14], s_fwd.at[index, block], to).start()

    wm_quarter = wm.at[quarter, :]
    weight_share = [
        remote(wm_quarter, wq.at[at(c * 128, 128), :], snd.at[11], s_wp.at[0], partner),
        remote(wdq.at[down_rows, :], wdq.at[down_rows, :], snd.at[12], s_wp.at[1], partner),
    ]

    @pl.when(jnp.logical_not(source))
    def _():
        got(wm_quarter, s_wy.at[0])
        got(wdq.at[down_rows, :], s_wy.at[1])
        for copy in weight_share:
            copy.start()
        for way, to in enumerate((right, left)):
            remote(wm_quarter, wm_quarter, snd.at[16], s_wr.at[way], (z, to, c, y)).start()

    spread(q_in, qf, snd.at[10], s_qr, 0, HALF)

    for load in loads:
        load.wait()
    for index, dst in enumerate((kp, vp)):
        for core in range(2):
            got(dst.at[core * 64 : (core + 1) * 64, :], s_hp.at[index, core])
    for index, dst in enumerate((kf, vf, qf)):
        got(dst.at[at((2 * x + p) * 64, 64), :], s_par.at[index])

    for block in range(NBLK):
        span = slice(block * BLK, (block + 1) * BLK)
        kt[block * BLK : (block + 1) * BLK, :] = kp[:, span].T
        kt[HALF + block * BLK : HALF + (block + 1) * BLK, :] = kf[quarter, span].T

    row_at = lax.broadcasted_iota(jnp.int32, (BLK, BLK), 0)
    col_at = lax.broadcasted_iota(jnp.int32, (BLK, BLK), 1)

    def attend(block):
        first = block * BLK
        asked = qf[quarter, first : first + BLK]
        top = jnp.full((1, BLK), -jnp.inf, F32)
        for part in range(5):
            key = first + part * BLK
            scores = dot(kt[key : key + BLK, :], asked) * SCALE
            if part == 0:
                scores = jnp.where(row_at > col_at, scores, -jnp.inf)
            if part == 4:
                scores = jnp.where(row_at <= col_at, scores, -jnp.inf)
            sc[part * BLK : (part + 1) * BLK, :] = scores
            top = jnp.maximum(top, jnp.max(scores, axis=0, keepdims=True))
        total = jnp.zeros((1, BLK), F32)
        blend = jnp.zeros((128, BLK), F32)
        for part in range(5):
            key = first + part * BLK
            raised = jnp.exp2(sc[part * BLK : (part + 1) * BLK, :] - top)
            total = total + jnp.sum(raised, axis=0, keepdims=True)
            if key < HALF:
                held = vp[:, key : key + BLK]
            else:
                held = vf[quarter, key - HALF : key - HALF + BLK]
            blend = blend + dot(held, raised.astype(BF16))
        ao[:, first : first + BLK] = (blend / total).astype(BF16)

    attend(0)

    for core, (first, second) in enumerate(((g_in, l_in), (l_in, g_in))):

        @pl.when(source & (c == core))
        def _():
            for load in full_weights(first, second):
                load.wait()

    @pl.when(jnp.logical_not(source))
    def _():
        got(wq.at[at(p * 128, 128), :], s_wp.at[0])
        got(wdq.at[at(p * 256, 256), :], s_wp.at[1])

    wq[at(c * 128, 128), :] = wm[quarter, :]
    for block in range(4):
        wdt[:, block * 128 : (block + 1) * 128] = wdq[block * 128 : (block + 1) * 128, :].T

    gd[...] = jnp.zeros_like(gd)
    for block in range(NBLK):
        span = slice(block * BLK, (block + 1) * BLK)
        for index, dst in enumerate((kf, vf)):
            got(dst.at[at(chips[1 - index] * 128, 128), span], s_ring.at[index, block, 1 - index])
            got(dst.at[at(far * 128, 128), span], s_fwd.at[index, block])
        keys = kf[:, span]
        rate = rt[pl.ds(z, 1), span]
        target = (-(vf[:, span].astype(F32) * rate)).astype(BF16)
        pre_gate = dot(wq[0:128, :], keys)
        pre_lift = dot(wq[128:256, :], keys)
        back = dot(wdt[...], target)
        sig = 1.0 / (1.0 + jnp.exp(-pre_gate))
        silu = pre_gate * sig
        hidden = (silu * pre_lift).astype(BF16)
        back_lift = (back * silu).astype(BF16)
        back_gate = (back * pre_lift * sig * (1.0 + pre_gate * (1.0 - sig))).astype(BF16)
        gd[0:128, :] += dot_t(back_gate, keys)
        gd[128:256, :] += dot_t(back_lift, keys)
        gd[256:384, :] += dot_t(hidden, target)

    main, down = slice(0, 128), slice(128, 192)
    ps[main, :] = gd[at(p * 128, 128), :].astype(BF16)
    remote(ps.at[main, :], pr.at[main, :], snd.at[15], s_rsp.at[0], partner).start()
    ps[down, :] = gd[at(256 + p * 64, 64), :].astype(BF16)
    remote(ps.at[down, :], pr.at[down, :], snd.at[28], s_rsp.at[1], partner).start()
    attend(1)

    def pair_and_send(index, span, first, size, low):
        got(pr.at[span, :], s_rsp.at[index])
        rows = slice(low, low + size)
        for owner in range(4):
            begin_at = span.start + owner * size
            both = gd[at(first + owner * size, size), :] + pr[
                begin_at : begin_at + size, :
            ].astype(F32)
            gs[owner, rows, :] = both.astype(BF16)
            ls[begin_at : begin_at + size, :] = both
        for step in (2, 1, 3):
            owner = lax.rem(y + step, 4)
            remote(
                gs.at[owner, rows, :],
                rr.at[y, rows, :],
                snd.at[17 + 10 * index],
                s_rs.at[index],
                (z, x, c, owner),
            ).start()

    def summed(index, span, size, low):
        rows = slice(low, low + size)
        got(rr.at[0:3, rows, :], s_rs.at[index])
        whole = ls[at(span.start + y * size, size), :]
        for step in range(1, 4):
            whole = whole + rr[lax.rem(y + step, 4), rows, :].astype(F32)
        return whole.astype(BF16)

    pair_and_send(0, main, c * 128, 32, 0)
    pair_and_send(1, down, 256 + c * 64, 16, 32)
    attend(2)
    attend(3)
    local(ao.at[own, :], att.at[:, half], s_loc.at[4]).start()
    give = remote(ao.at[theirs, :], att.at[:, half], snd.at[23], s_oa, partner)
    give.start()
    ym[4 * x + y] = summed(0, main, 32, 0)

    def gather(ref, index, ways, recv_low, recv_high, send):
        for step in (2, 1, 3):
            in_y = (z, x, c, lax.rem(y + step, 4))
            in_x = (z, lax.rem(x + step, 4), c, y)
            low, high = ref.at[index, :, 0:256], ref.at[index, :, 256:512]
            to_low, to_high = (in_y, in_x) if ways == 0 else (in_x, in_y)
            remote(low, low, send, recv_low(step), to_low).start()
            remote(high, high, send, recv_high(step), to_high).start()

    def gather_first(ref, index, first, send):
        gather(ref, index, 0, lambda n: first.at[0, n], lambda n: first.at[1, n], send)

    def gather_rest(ref, index, second, send):
        gather(ref, index, 1, lambda n: second, lambda n: second, send)

    def relay(ref, index_of, first, second, send):
        low, high = slice(0, 256), slice(256, 512)
        for step in (1, 3, 2):
            across = index_of(x, lax.rem(y + 4 - step, 4))
            part = ref.at[across, :, low]
            got(part, first.at[0, step])
            for hop in (2, 1, 3):
                to = (z, lax.rem(x + hop, 4), c, y)
                remote(part, part, send, second, to).start()
            along = index_of(lax.rem(x + 4 - step, 4), y)
            part = ref.at[along, :, high]
            got(part, first.at[1, step])
            for hop in (2, 1, 3):
                to = (z, x, c, lax.rem(y + hop, 4))
                remote(part, part, send, second, to).start()

    def main_at(xx, yy):
        return 4 * xx + yy

    def down_at(xx, yy):
        return 4 * (2 * xx + c) + yy

    gather_first(ym, main_at(x, y), s_ag, snd.at[18])
    gather_rest(ym, main_at(x, y), s_ag2, snd.at[18])
    yd[down_at(x, y)] = summed(1, down, 16, 32)
    gather_first(yd, down_at(x, y), s_dag, snd.at[19])
    relay(ym, main_at, s_ag, s_ag2, snd.at[18])
    gather_rest(yd, down_at(x, y), s_dag2, snd.at[19])
    relay(yd, down_at, s_dag, s_dag2, snd.at[19])

    @pl.when(jnp.logical_not(source))
    def _():
        for way in range(2):
            got(wm_quarter, s_wr.at[way])
        for index in range(2):
            part = wm.at[at(chips[index] * 128 + index * 64, 64), :]
            to = (z, chips[1 - index], c, y)
            remote(part, part, snd.at[21], s_wf.at[index], to).start()
        got(wdr.at[own, :], s_wy.at[2])
        remote(wdr.at[own, :], wdr.at[own, :], snd.at[22], s_wp.at[2], partner).start()

    for way in range(2):
        got(qf.at[at(chips[way] * 128, 128), :], s_qr.at[way])
        part = qf.at[at(chips[way] * 128, 128), way * 512 : way * 512 + 512]
        to = (z, chips[1 - way], c, y)
        remote(part, part, snd.at[7], s_qfw.at[way], to).start()

    def begin(rounded):
        wide = rounded.astype(F32)
        norm = jnp.sqrt(jnp.sum(jnp.square(wide), keepdims=True) + EPS)
        return (wide / norm).astype(BF16)

    def sweep():
        zs[...] = dot_t(xs[...], xs[...]).astype(BF16)
        fd[...] = dot(zs[...], xs[...]).astype(BF16)
        xs[...] = (
            COEF_A * xs[...].astype(F32)
            + COEF_B * fd[...].astype(F32)
            + COEF_C * dot(zs[...], fd[...])
        ).astype(BF16)

    def fresh(weight, turned):
        initial = weight.astype(F32)
        moved = initial - turned.astype(F32)
        wanted = jnp.sqrt(jnp.mean(jnp.square(initial), axis=-1, keepdims=True) + EPS)
        present = jnp.sqrt(jnp.mean(jnp.square(moved), axis=-1, keepdims=True) + EPS)
        return (moved * (wanted / present)).astype(BF16)

    got(ym.at[0:12], s_ag2)
    xs[...] = begin(ym[...].reshape(512, 512))
    sweep()
    sweep()

    got(yd.at[0:12], s_dag2)
    halves = [yd.at[at(8 * chip + 4 * c, 4)] for chip in range(4)]
    for chip in range(4):
        remote(halves[chip], halves[chip], snd.at[20], s_dp, partner).start()

    @pl.when(jnp.logical_not(source))
    def _():
        for index in range(2):
            got(wm.at[at(far * 128 + index * 64, 64), :], s_wf.at[index])

    fr[c] = fresh(wm[...], xs[...])
    lend = remote(fr.at[c], fr.at[c], snd.at[13], s_fr, partner)
    lend.start()

    got(yd.at[0:16], s_dp)
    xs[...] = begin(yd[...].reshape(512, 512))
    sweep()
    zs[...] = dot_t(xs[...], xs[...]).astype(BF16)
    side = xs[:, quarter]
    lifted = dot(zs[...], side).astype(BF16)
    turned = (
        COEF_A * side.astype(F32) + COEF_B * lifted.astype(F32) + COEF_C * dot(zs[...], lifted)
    ).astype(BF16)

    @pl.when(jnp.logical_not(source))
    def _():
        got(wdr.at[theirs, :], s_wp.at[2])

    wdt[...] = fresh(wdr[...], turned.T)

    for way in range(2):
        got(qf.at[at(far * 128, 128), way * 512 : way * 512 + 512], s_qfw.at[way])
    got(fr.at[p], s_fr)
    for block in range(NBLK):
        span = slice(block * BLK, (block + 1) * BLK)
        asked = qf[:, span]
        query_gate = dot(fr[0], asked)
        query_lift = dot(fr[1], asked)
        query_hidden = (query_gate / (1.0 + jnp.exp(-query_gate)) * query_lift).astype(BF16)
        ro[:, span] = dot(wdt[...], query_hidden).astype(BF16)
        here = at(c * HALF + block * BLK, BLK)
        remote(ro.at[theirs, span], rec.at[:, here], snd.at[24], s_or, partner).start()
        local(ro.at[own, span], rec.at[:, here], s_loc.at[5 + block]).start()

    def drain(ref, index):
        remote(ref, ref, snd.at[index], s_or, partner).wait_send()

    for block in range(NBLK):
        span = slice(block * BLK, (block + 1) * BLK)
        local(ro.at[own, span], ro.at[own, span], s_loc.at[5 + block]).wait()
    local(ao.at[own, :], att.at[:, half], s_loc.at[4]).wait()
    give.wait_send()
    got(ao.at[own, :], s_oa)
    lend.wait_send()
    for copy in share:
        copy.wait_send()

    @pl.when(c == 0)
    def _():
        for copy in within:
            copy.wait_send()

    @pl.when((c == 1) & (y == 0))
    def _():
        for copy in cached:
            copy.wait_send()

    @pl.when(y < 3)
    def _():
        for copy in halo:
            copy.wait_send()

    @pl.when(source)
    def _():
        drain(kf.at[0:288, :], 0)
        drain(wm.at[0:192, :], 6)

    for index in range(2):
        drain(kf.at[0:256, :], 8 + index)
    drain(kf.at[0:256, :], 14)
    drain(kf.at[0:256, :], 10)
    drain(kf.at[0:128, :], 7)

    @pl.when(jnp.logical_not(source))
    def _():
        for copy in weight_share:
            copy.wait_send()
        drain(wm.at[0:256, :], 16)
        drain(wm.at[0:128, :], 21)
        drain(wdr.at[own, :], 22)

    drain(pr.at[main, :], 15)
    drain(pr.at[down, :], 28)
    drain(rr.at[0:3, 0:32], 17)
    drain(rr.at[0:3, 32:48], 27)
    drain(ym.at[0:15], 18)
    drain(yd.at[0:15], 19)
    drain(yd.at[0:16], 20)
    drain(ro.at[0:64, :], 24)
    got(ro.at[0:64, :], s_or)


def write_out(att, rec, att_out, rec_out, sem):
    copies = [local(att, att_out, sem.at[0]), local(rec, rec_out, sem.at[1])]
    for copy in copies:
        copy.start()
    for copy in copies:
        copy.wait()


def per_device(*arrays):
    any_spec = pl.BlockSpec(memory_space=pl.ANY)
    out = pltpu.VMEM((64, 2 * HALF), BF16)
    arrays = [pltpu.with_memory_space_constraint(a, pltpu.HBM) for a in arrays]
    vmem = pltpu.VMEM
    dma = pltpu.SemaphoreType.DMA
    held = pl.pallas_call(
        kernel,
        out_shape=(out, out),
        in_specs=[any_spec] * 9,
        out_specs=(any_spec, any_spec),
        scratch_shapes=[
            vmem((512, HALF), BF16),
            vmem((512, HALF), BF16),
            vmem((512, HALF), BF16),
            vmem((128, HALF), BF16),
            vmem((128, HALF), BF16),
            vmem((512, 512), BF16),
            vmem((256, 512), BF16),
            vmem((512, 128), BF16),
            vmem((128, 512), BF16),
            vmem((128, 512), BF16),
            vmem((2 * HALF, 128), BF16),
            vmem((5 * BLK, BLK), F32),
            vmem((128, HALF), BF16),
            vmem((384, 512), F32),
            vmem((192, 512), BF16),
            vmem((192, 512), BF16),
            vmem((4, 48, 512), BF16),
            vmem((4, 48, 512), BF16),
            vmem((16, 32, 512), BF16),
            vmem((32, 16, 512), BF16),
            vmem((512, 512), BF16),
            vmem((512, 512), BF16),
            vmem((192, 512), F32),
            vmem((2, 512, 512), BF16),
            vmem((512, 512), BF16),
            vmem((128, HALF), BF16),
            vmem((8, HALF), F32),
            dma((9,)),
            dma((2, 2)),
            dma((3,)),
            dma((2, NBLK, 2)),
            dma((2, NBLK)),
            dma((4,)),
            dma((3,)),
            dma((2,)),
            dma((2,)),
            dma((2,)),
            dma((2,)),
            dma((2,)),
            dma((2,)),
            dma((2, 4)),
            dma(()),
            dma((2, 4)),
            dma(()),
            dma(()),
            dma(()),
            dma(()),
            dma(()),
            dma((29,)),
        ],
        compiler_params=pltpu.CompilerParams(
            collective_id=0, has_side_effects=True, vmem_limit_bytes=48000000
        ),
        name="plane",
    )(*arrays)
    return pl.pallas_call(
        write_out,
        out_shape=(pltpu.HBM((64, 2 * HALF), BF16),) * 2,
        in_specs=[pl.BlockSpec(memory_space=vmem)] * 2,
        out_specs=(pl.BlockSpec(memory_space=pltpu.HBM),) * 2,
        scratch_shapes=[dma((2,))],
        name="write_out",
    )(*[pltpu.with_memory_space_constraint(a, pltpu.VMEM) for a in held])


def solution(mesh):
    split = Mesh(mesh.devices.reshape(8, 4, 2, 4), ("z", "x", "c", "y"))
    tokens = P(WIDE, "y")
    heads = P("y", None, None)
    return jax.shard_map(
        per_device,
        mesh=split,
        in_specs=(tokens, tokens, tokens, P(WIDE), P(WIDE), heads, heads, heads, P()),
        out_specs=(tokens, tokens),
        check_vma=False,
    )
```

```python
import functools
import math

import jax
import jax.numpy as jnp
from jax import lax
from jax.experimental import pallas as pl
from jax.experimental.pallas import tpu as pltpu
from jax.sharding import Mesh
from jax.sharding import PartitionSpec as P

WIDE = ("z", "x", "c")
EPS = 1e-06
COEF_A = 3.4445
COEF_B = -4.775
COEF_C = 2.0315
HALF = 1024
BLK = 256
NBLK = HALF // BLK
SCALE = math.log2(math.e) / math.sqrt(128)
F32 = jnp.float32
BF16 = jnp.bfloat16


def dot(a, b):
    return lax.dot_general(a, b, (((1,), (0,)), ((), ())), preferred_element_type=F32)


def dot_t(a, b):
    return lax.dot_general(a, b, (((1,), (1,)), ((), ())), preferred_element_type=F32)


def local(src, dst, sem):
    return pltpu.make_async_copy(src, dst, sem)


def remote(src, dst, send, recv, device):
    return pltpu.make_async_remote_copy(
        src_ref=src,
        dst_ref=dst,
        send_sem=send,
        recv_sem=recv,
        device_id=device,
        device_id_type=pl.DeviceIdType.MESH,
    )


def kernel(
    q_in, k_in, v_in, ck_in, cv_in, g_in, l_in, d_in, r_in,
    att, rec,
    kf, vf, qf, kp, vp, wm, wq, wdq, wdr, wdt, kt, sc, ao, gd, ps, pr, gs, rr, ym, yd, xs, zs, ls,
    fr, fd, ro, rt, hq,
    s_loc, s_hp, s_par, s_ring, s_fwd, s_wy, s_wp, s_wr, s_wf, s_qr, s_qfw, s_rsp, s_rs, s_ag, s_ag2,
    s_dag, s_dag2, s_dp, s_fr, s_oa, s_or, snd,
):
    z = lax.axis_index("z")
    x = lax.axis_index("x")
    c = lax.axis_index("c")
    y = lax.axis_index("y")
    p = 1 - c
    right = lax.rem(x + 1, 4)
    left = lax.rem(x + 3, 4)
    far = lax.rem(x + 2, 4)
    me = 2 * x + c
    head = lax.rem(z, 2)
    source = y == z // 2
    partner = (z, x, p, y)

    def at(start, size):
        return pl.ds(pl.multiple_of(start, size), size)

    mine = at(me * 64, 64)
    half = at(c * HALF, HALF)
    other = at(p * HALF, HALF)
    own = at(c * 64, 64)
    theirs = at(p * 64, 64)
    quarter = at(x * 128, 128)
    down_rows = at(c * 256, 256)
    down_piece = at(x * 128 + c * 64, 64)

    def got(ref, sem):
        remote(ref, ref, snd.at[0], sem, partner).wait_recv()

    loads = [
        local(k_in.at[:, half], kf.at[mine, :], s_loc.at[0]),
        local(v_in.at[:, half], vf.at[mine, :], s_loc.at[1]),
        local(q_in.at[:, half], qf.at[mine, :], s_loc.at[2]),
        local(r_in.at[:, at(y * 2 * HALF + c * HALF, HALF)], rt, s_loc.at[3]),
    ]
    for load in loads:
        load.start()

    @pl.when(c == 1)
    def _():
        local(k_in.at[:, :HALF], kp.at[own, :], s_hp.at[0, c]).start()
        local(v_in.at[:, :HALF], vp.at[own, :], s_hp.at[1, c]).start()

    @pl.when((c == 0) & (y == 0))
    def _():
        local(ck_in, kp.at[own, :], s_hp.at[0, c]).start()
        local(cv_in, vp.at[own, :], s_hp.at[1, c]).start()

    def full_weights(first, second):
        return [
            local(first.at[head], wm, s_wy.at[0]),
            local(second.at[head, quarter, :], wq.at[at(p * 128, 128), :], s_wy.at[1]),
            local(d_in.at[head, :, quarter], wdq, s_wy.at[2]),
            local(d_in.at[head, quarter, :], wdr, s_wy.at[3]),
        ]

    for core, (first, second) in enumerate(((g_in, l_in), (l_in, g_in))):

        @pl.when(source & (c == core))
        def _():
            for load in full_weights(first, second):
                load.start()

    barrier = pltpu.get_barrier_semaphore()
    peers = [partner]
    for step in range(1, 4):
        for core in range(2):
            peers.append((z, lax.rem(x + step, 4), core, y))
            peers.append((z, x, core, lax.rem(y + step, 4)))
    for peer in peers:
        pl.semaphore_signal(barrier, inc=1, device_id=peer, device_id_type=pl.DeviceIdType.MESH)
    pl.semaphore_wait(barrier, len(peers))

    for core, first in enumerate((g_in, l_in)):

        @pl.when(source & (c == core))
        def _():
            for step in (2, 1, 3):
                to = (z, x, c, lax.rem(y + step, 4))
                remote(
                    first.at[head, quarter, :], wm.at[quarter, :], snd.at[0], s_wy.at[0], to
                ).start()
                remote(
                    d_in.at[head, down_rows, quarter],
                    wdq.at[down_rows, :],
                    snd.at[0],
                    s_wy.at[1],
                    to,
                ).start()

    share = [
        remote(k_in.at[:, other], kf.at[mine, :], snd.at[1], s_par.at[0], partner),
        remote(v_in.at[:, other], vf.at[mine, :], snd.at[2], s_par.at[1], partner),
        remote(q_in.at[:, other], qf.at[mine, :], snd.at[3], s_par.at[2], partner),
    ]
    for copy in share:
        copy.start()

    def prior(ks, vs, to, index):
        return [
            remote(ks, kp.at[own, :], snd.at[index], s_hp.at[0, c], to),
            remote(vs, vp.at[own, :], snd.at[index + 1], s_hp.at[1, c], to),
        ]

    within = prior(k_in.at[:, :HALF], v_in.at[:, :HALF], partner, 4)
    cached = prior(ck_in, cv_in, partner, 4)
    halo = prior(k_in.at[:, HALF:], v_in.at[:, HALF:], (z, x, 0, lax.rem(y + 1, 4)), 25)

    @pl.when(c == 0)
    def _():
        for copy in within:
            copy.start()

    @pl.when((c == 1) & (y == 0))
    def _():
        for copy in cached:
            copy.start()

    def spread(src, dst, send, recv, first, size):
        for way, to in enumerate((right, left)):
            for core in range(2):
                remote(
                    src.at[:, core * HALF + first : core * HALF + first + size],
                    dst.at[mine, first : first + size],
                    send,
                    recv.at[way],
                    (z, to, core, y),
                ).start()

    for block in range(NBLK):
        for index, (src, dst) in enumerate(((k_in, kf), (v_in, vf))):
            spread(src, dst, snd.at[8 + index], s_ring.at[index, block], block * BLK, BLK)

    @pl.when(y < 3)
    def _():
        for copy in halo:
            copy.start()

    @pl.when(source)
    def _():
        for step in (2, 1, 3):
            to = (z, x, c, lax.rem(y + step, 4))
            remote(
                d_in.at[head, down_piece, :], wdr.at[own, :], snd.at[6], s_wy.at[2], to
            ).start()

    chips = (left, right)
    for block in range(NBLK):
        span = slice(block * BLK, (block + 1) * BLK)
        for index, dst in enumerate((kf, vf)):
            part = dst.at[at(chips[index] * 128, 128), span]
            got(part, s_ring.at[index, block, index])
            to = (z, chips[1 - index], c, y)
            remote(part, part, snd.at[14], s_fwd.at[index, block], to).start()

    wm_quarter = wm.at[quarter, :]
    weight_share = [
        remote(wm_quarter, wq.at[at(c * 128, 128), :], snd.at[11], s_wp.at[0], partner),
        remote(wdq.at[down_rows, :], wdq.at[down_rows, :], snd.at[12], s_wp.at[1], partner),
    ]

    @pl.when(jnp.logical_not(source))
    def _():
        got(wm_quarter, s_wy.at[0])
        got(wdq.at[down_rows, :], s_wy.at[1])
        for copy in weight_share:
            copy.start()
        for way, to in enumerate((right, left)):
            remote(wm_quarter, wm_quarter, snd.at[16], s_wr.at[way], (z, to, c, y)).start()

    spread(q_in, qf, snd.at[10], s_qr, 0, HALF)

    for load in loads:
        load.wait()
    for index, dst in enumerate((kp, vp)):
        for core in range(2):
            got(dst.at[core * 64 : (core + 1) * 64, :], s_hp.at[index, core])
    for index, dst in enumerate((kf, vf, qf)):
        got(dst.at[at((2 * x + p) * 64, 64), :], s_par.at[index])

    for block in range(NBLK):
        span = slice(block * BLK, (block + 1) * BLK)
        kt[block * BLK : (block + 1) * BLK, :] = kp[:, span].T
        kt[HALF + block * BLK : HALF + (block + 1) * BLK, :] = kf[quarter, span].T

    row_at = lax.broadcasted_iota(jnp.int32, (BLK, BLK), 0)
    col_at = lax.broadcasted_iota(jnp.int32, (BLK, BLK), 1)

    def attend(block):
        first = block * BLK
        asked = qf[quarter, first : first + BLK]
        top = jnp.full((1, BLK), -jnp.inf, F32)
        for part in range(5):
            key = first + part * BLK
            scores = dot(kt[key : key + BLK, :], asked) * SCALE
            if part == 0:
                scores = jnp.where(row_at > col_at, scores, -jnp.inf)
            if part == 4:
                scores = jnp.where(row_at <= col_at, scores, -jnp.inf)
            sc[part * BLK : (part + 1) * BLK, :] = scores
            top = jnp.maximum(top, jnp.max(scores, axis=0, keepdims=True))
        total = jnp.zeros((1, BLK), F32)
        blend = jnp.zeros((128, BLK), F32)
        for part in range(5):
            key = first + part * BLK
            raised = jnp.exp2(sc[part * BLK : (part + 1) * BLK, :] - top)
            total = total + jnp.sum(raised, axis=0, keepdims=True)
            if key < HALF:
                held = vp[:, key : key + BLK]
            else:
                held = vf[quarter, key - HALF : key - HALF + BLK]
            blend = blend + dot(held, raised.astype(BF16))
        ao[:, first : first + BLK] = (blend / total).astype(BF16)

    attend(0)

    for core, (first, second) in enumerate(((g_in, l_in), (l_in, g_in))):

        @pl.when(source & (c == core))
        def _():
            for load in full_weights(first, second):
                load.wait()

    @pl.when(jnp.logical_not(source))
    def _():
        got(wq.at[at(p * 128, 128), :], s_wp.at[0])
        got(wdq.at[at(p * 256, 256), :], s_wp.at[1])

    wq[at(c * 128, 128), :] = wm[quarter, :]
    for block in range(4):
        wdt[:, block * 128 : (block + 1) * 128] = wdq[block * 128 : (block + 1) * 128, :].T

    gd[...] = jnp.zeros_like(gd)
    for block in range(NBLK):
        span = slice(block * BLK, (block + 1) * BLK)
        for index, dst in enumerate((kf, vf)):
            got(dst.at[at(chips[1 - index] * 128, 128), span], s_ring.at[index, block, 1 - index])
            got(dst.at[at(far * 128, 128), span], s_fwd.at[index, block])
        keys = kf[:, span]
        rate = rt[pl.ds(z, 1), span]
        target = (-(vf[:, span].astype(F32) * rate)).astype(BF16)
        pre_gate = dot(wq[0:128, :], keys)
        pre_lift = dot(wq[128:256, :], keys)
        back = dot(wdt[...], target)
        sig = 1.0 / (1.0 + jnp.exp(-pre_gate))
        silu = pre_gate * sig
        hidden = (silu * pre_lift).astype(BF16)
        back_lift = (back * silu).astype(BF16)
        back_gate = (back * pre_lift * sig * (1.0 + pre_gate * (1.0 - sig))).astype(BF16)
        gd[0:128, :] += dot_t(back_gate, keys)
        gd[128:256, :] += dot_t(back_lift, keys)
        gd[256:384, :] += dot_t(hidden, target)

    main, down = slice(0, 128), slice(128, 256)
    ps[main, :] = gd[at(p * 128, 128), :].astype(BF16)
    remote(ps.at[main, :], pr.at[main, :], snd.at[15], s_rsp.at[0], partner).start()

    @pl.when(c == 0)
    def _():
        ps[down, :] = gd[256:384, :].astype(BF16)
        remote(ps.at[down, :], pr.at[down, :], snd.at[28], s_rsp.at[1], partner).start()

    attend(1)

    def pair_and_send(index, span, first, size, low):
        got(pr.at[span, :], s_rsp.at[index])
        rows = slice(low, low + size)
        for owner in range(4):
            begin_at = span.start + owner * size
            both = gd[at(first + owner * size, size), :] + pr[
                begin_at : begin_at + size, :
            ].astype(F32)
            gs[owner, rows, :] = both.astype(BF16)
            ls[begin_at : begin_at + size, :] = both
        for step in (2, 1, 3):
            owner = lax.rem(y + step, 4)
            remote(
                gs.at[owner, rows, :],
                rr.at[y, rows, :],
                snd.at[17 + 10 * index],
                s_rs.at[index],
                (z, x, c, owner),
            ).start()

    def summed(index, span, size, low):
        rows = slice(low, low + size)
        got(rr.at[0:3, rows, :], s_rs.at[index])
        whole = ls[at(span.start + y * size, size), :]
        for step in range(1, 4):
            whole = whole + rr[lax.rem(y + step, 4), rows, :].astype(F32)
        return whole.astype(BF16)

    pair_and_send(0, main, c * 128, 32, 0)

    @pl.when(c == 1)
    def _():
        pair_and_send(1, down, 256, 32, 32)

    attend(2)
    attend(3)
    local(ao.at[own, :], att.at[:, half], s_loc.at[4]).start()
    give = remote(ao.at[theirs, :], att.at[:, half], snd.at[23], s_oa, partner)
    give.start()
    ym[4 * x + y] = summed(0, main, 32, 0)

    def gather(ref, index, ways, recv_low, recv_high, send):
        for step in (2, 1, 3):
            in_y = (z, x, c, lax.rem(y + step, 4))
            in_x = (z, lax.rem(x + step, 4), c, y)
            low, high = ref.at[index, :, 0:256], ref.at[index, :, 256:512]
            to_low, to_high = (in_y, in_x) if ways == 0 else (in_x, in_y)
            remote(low, low, send, recv_low(step), to_low).start()
            remote(high, high, send, recv_high(step), to_high).start()

    def gather_first(ref, index, first, send):
        gather(ref, index, 0, lambda n: first.at[0, n], lambda n: first.at[1, n], send)

    def gather_rest(ref, index, second, send):
        gather(ref, index, 1, lambda n: second, lambda n: second, send)

    def relay(ref, index_of, first, second, send):
        low, high = slice(0, 256), slice(256, 512)
        for step in (1, 3, 2):
            across = index_of(x, lax.rem(y + 4 - step, 4))
            part = ref.at[across, :, low]
            got(part, first.at[0, step])
            for hop in (2, 1, 3):
                to = (z, lax.rem(x + hop, 4), c, y)
                remote(part, part, send, second, to).start()
            along = index_of(lax.rem(x + 4 - step, 4), y)
            part = ref.at[along, :, high]
            got(part, first.at[1, step])
            for hop in (2, 1, 3):
                to = (z, x, c, lax.rem(y + hop, 4))
                remote(part, part, send, second, to).start()

    def main_at(xx, yy):
        return 4 * xx + yy

    place = main_at(x, y)
    gather_first(ym, place, s_ag, snd.at[18])
    gather_rest(ym, place, s_ag2, snd.at[18])

    @pl.when(c == 1)
    def _():
        yd[place] = summed(1, down, 32, 32)
        gather_first(yd, place, s_dag, snd.at[19])

    relay(ym, main_at, s_ag, s_ag2, snd.at[18])

    @pl.when(c == 1)
    def _():
        gather_rest(yd, place, s_dag2, snd.at[19])
        relay(yd, main_at, s_dag, s_dag2, snd.at[19])

    @pl.when(jnp.logical_not(source))
    def _():
        for way in range(2):
            got(wm_quarter, s_wr.at[way])
        for index in range(2):
            part = wm.at[at(chips[index] * 128 + index * 64, 64), :]
            to = (z, chips[1 - index], c, y)
            remote(part, part, snd.at[21], s_wf.at[index], to).start()
        got(wdr.at[own, :], s_wy.at[2])
        remote(wdr.at[own, :], wdr.at[own, :], snd.at[22], s_wp.at[2], partner).start()

    for way in range(2):
        rows = at(chips[way] * 128, 128)
        got(qf.at[rows, :], s_qr.at[way])
        part = qf.at[rows, way * 512 : way * 512 + 512]
        remote(part, part, snd.at[7], s_qfw.at[way], (z, chips[1 - way], c, y)).start()

    def begin(rounded):
        wide = rounded.astype(F32)
        norm = jnp.sqrt(jnp.sum(jnp.square(wide), keepdims=True) + EPS)
        return (wide / norm).astype(BF16)

    def sweep():
        zs[...] = dot_t(xs[...], xs[...]).astype(BF16)
        fd[...] = dot(zs[...], xs[...]).astype(BF16)
        xs[...] = (
            COEF_A * xs[...].astype(F32)
            + COEF_B * fd[...].astype(F32)
            + COEF_C * dot(zs[...], fd[...])
        ).astype(BF16)

    def fresh(weight, turned):
        initial = weight.astype(F32)
        moved = initial - turned.astype(F32)
        wanted = jnp.sqrt(jnp.mean(jnp.square(initial), axis=-1, keepdims=True) + EPS)
        present = jnp.sqrt(jnp.mean(jnp.square(moved), axis=-1, keepdims=True) + EPS)
        return (moved * (wanted / present)).astype(BF16)

    got(ym.at[0:12], s_ag2)
    xs[...] = begin(ym[...].reshape(512, 512))
    sweep()
    sweep()

    @pl.when(jnp.logical_not(source))
    def _():
        for index in range(2):
            got(wm.at[at(far * 128 + index * 64, 64), :], s_wf.at[index])

    fr[c] = fresh(wm[...], xs[...])
    lend = remote(fr.at[c], fr.at[c], snd.at[13], s_fr, partner)
    lend.start()

    @pl.when(jnp.logical_not(source))
    def _():
        got(wdr.at[theirs, :], s_wp.at[2])

    lend_down = remote(fd.at[0:128, :], wdt, snd.at[20], s_dp, partner)

    @pl.when(c == 1)
    def _():
        got(yd.at[0:12], s_dag2)
        xs[...] = begin(yd[...].reshape(512, 512))
        sweep()
        zs[...] = dot_t(xs[...], xs[...]).astype(BF16)
        side = xs[:, quarter]
        lifted = dot(zs[...], side).astype(BF16)
        turned = (
            COEF_A * side.astype(F32) + COEF_B * lifted.astype(F32) + COEF_C * dot(zs[...], lifted)
        ).astype(BF16)
        new = fresh(wdr[...], turned.T)
        fd[0:128, :] = new
        wdt[...] = new
        lend_down.start()

    for way in range(2):
        got(qf.at[at(far * 128, 128), way * 512 : way * 512 + 512], s_qfw.at[way])
    got(fr.at[p], s_fr)

    def hide(block):
        span = slice(block * BLK, (block + 1) * BLK)
        asked = qf[:, span]
        query_gate = dot(fr[0], asked)
        query_lift = dot(fr[1], asked)
        return (query_gate / (1.0 + jnp.exp(-query_gate)) * query_lift).astype(BF16)

    def settle(block, hidden):
        span = slice(block * BLK, (block + 1) * BLK)
        ro[:, span] = dot(wdt[...], hidden).astype(BF16)
        here = at(c * HALF + block * BLK, BLK)
        remote(ro.at[theirs, span], rec.at[:, here], snd.at[24], s_or, partner).start()
        local(ro.at[own, span], rec.at[:, here], s_loc.at[5 + block]).start()

    @pl.when(c == 0)
    def _():
        for block in range(NBLK):
            hq[:, block * BLK : (block + 1) * BLK] = hide(block)
        got(wdt, s_dp)
        for block in range(NBLK):
            settle(block, hq[:, block * BLK : (block + 1) * BLK])

    @pl.when(c == 1)
    def _():
        for block in range(NBLK):
            settle(block, hide(block))

    def drain(ref, index):
        remote(ref, ref, snd.at[index], s_or, partner).wait_send()

    for block in range(NBLK):
        span = slice(block * BLK, (block + 1) * BLK)
        local(ro.at[own, span], ro.at[own, span], s_loc.at[5 + block]).wait()
    local(ao.at[own, :], att.at[:, half], s_loc.at[4]).wait()
    give.wait_send()
    got(ao.at[own, :], s_oa)
    lend.wait_send()
    for copy in share:
        copy.wait_send()

    @pl.when(c == 0)
    def _():
        for copy in within:
            copy.wait_send()

    @pl.when((c == 1) & (y == 0))
    def _():
        for copy in cached:
            copy.wait_send()

    @pl.when(y < 3)
    def _():
        for copy in halo:
            copy.wait_send()

    @pl.when(source)
    def _():
        drain(kf.at[0:288, :], 0)
        drain(wm.at[0:192, :], 6)

    for index in range(2):
        drain(kf.at[0:256, :], 8 + index)
    drain(kf.at[0:256, :], 14)
    drain(kf.at[0:256, :], 10)
    drain(kf.at[0:128, :], 7)

    @pl.when(jnp.logical_not(source))
    def _():
        for copy in weight_share:
            copy.wait_send()
        drain(wm.at[0:256, :], 16)
        drain(wm.at[0:128, :], 21)
        drain(wdr.at[own, :], 22)

    drain(pr.at[main, :], 15)
    drain(rr.at[0:3, 0:32], 17)
    drain(ym.at[0:15], 18)

    @pl.when(c == 0)
    def _():
        drain(pr.at[down, :], 28)

    @pl.when(c == 1)
    def _():
        drain(rr.at[0:3, 32:64], 27)
        drain(yd.at[0:15], 19)
        lend_down.wait_send()

    drain(ro.at[0:64, :], 24)
    got(ro.at[0:64, :], s_or)


def write_out(att, rec, att_out, rec_out, sem):
    copies = [local(att, att_out, sem.at[0]), local(rec, rec_out, sem.at[1])]
    for copy in copies:
        copy.start()
    for copy in copies:
        copy.wait()


def per_device(*arrays):
    any_spec = pl.BlockSpec(memory_space=pl.ANY)
    out = pltpu.VMEM((64, 2 * HALF), BF16)
    arrays = [pltpu.with_memory_space_constraint(a, pltpu.HBM) for a in arrays]
    vmem = pltpu.VMEM
    dma = pltpu.SemaphoreType.DMA
    held = pl.pallas_call(
        kernel,
        out_shape=(out, out),
        in_specs=[any_spec] * 9,
        out_specs=(any_spec, any_spec),
        scratch_shapes=[
            vmem((512, HALF), BF16),
            vmem((512, HALF), BF16),
            vmem((512, HALF), BF16),
            vmem((128, HALF), BF16),
            vmem((128, HALF), BF16),
            vmem((512, 512), BF16),
            vmem((256, 512), BF16),
            vmem((512, 128), BF16),
            vmem((128, 512), BF16),
            vmem((128, 512), BF16),
            vmem((2 * HALF, 128), BF16),
            vmem((5 * BLK, BLK), F32),
            vmem((128, HALF), BF16),
            vmem((384, 512), F32),
            vmem((256, 512), BF16),
            vmem((256, 512), BF16),
            vmem((4, 64, 512), BF16),
            vmem((4, 64, 512), BF16),
            vmem((16, 32, 512), BF16),
            vmem((16, 32, 512), BF16),
            vmem((512, 512), BF16),
            vmem((512, 512), BF16),
            vmem((256, 512), F32),
            vmem((2, 512, 512), BF16),
            vmem((512, 512), BF16),
            vmem((128, HALF), BF16),
            vmem((8, HALF), F32),
            vmem((512, HALF), BF16),
            dma((9,)),
            dma((2, 2)),
            dma((3,)),
            dma((2, NBLK, 2)),
            dma((2, NBLK)),
            dma((4,)),
            dma((3,)),
            dma((2,)),
            dma((2,)),
            dma((2,)),
            dma((2,)),
            dma((2,)),
            dma((2,)),
            dma((2, 4)),
            dma(()),
            dma((2, 4)),
            dma(()),
            dma(()),
            dma(()),
            dma(()),
            dma(()),
            dma((29,)),
        ],
        compiler_params=pltpu.CompilerParams(
            collective_id=0, has_side_effects=True, vmem_limit_bytes=48000000
        ),
        name="plane",
    )(*arrays)
    return pl.pallas_call(
        write_out,
        out_shape=(pltpu.HBM((64, 2 * HALF), BF16),) * 2,
        in_specs=[pl.BlockSpec(memory_space=vmem)] * 2,
        out_specs=(pl.BlockSpec(memory_space=pltpu.HBM),) * 2,
        scratch_shapes=[dma((2,))],
        name="write_out",
    )(*[pltpu.with_memory_space_constraint(a, pltpu.VMEM) for a in held])


def solution(mesh):
    split = Mesh(mesh.devices.reshape(8, 4, 2, 4), ("z", "x", "c", "y"))
    tokens = P(WIDE, "y")
    heads = P("y", None, None)
    return jax.shard_map(
        per_device,
        mesh=split,
        in_specs=(tokens, tokens, tokens, P(WIDE), P(WIDE), heads, heads, heads, P()),
        out_specs=(tokens, tokens),
        check_vma=False,
    )
```

```python
import functools
import math

import jax
import jax.numpy as jnp
from jax import lax
from jax.experimental import pallas as pl
from jax.experimental.pallas import tpu as pltpu
from jax.sharding import Mesh
from jax.sharding import PartitionSpec as P

WIDE = ("z", "x", "c")
EPS = 1e-06
COEF_A = 3.4445
COEF_B = -4.775
COEF_C = 2.0315
HALF = 1024
BLK = 256
NBLK = HALF // BLK
SCALE = math.log2(math.e) / math.sqrt(128)
F32 = jnp.float32
BF16 = jnp.bfloat16


def dot(a, b):
    return lax.dot_general(a, b, (((1,), (0,)), ((), ())), preferred_element_type=F32)


def dot_t(a, b):
    return lax.dot_general(a, b, (((1,), (1,)), ((), ())), preferred_element_type=F32)


def local(src, dst, sem):
    return pltpu.make_async_copy(src, dst, sem)


def remote(src, dst, send, recv, device):
    return pltpu.make_async_remote_copy(
        src_ref=src,
        dst_ref=dst,
        send_sem=send,
        recv_sem=recv,
        device_id=device,
        device_id_type=pl.DeviceIdType.MESH,
    )


def kernel(
    q_in, k_in, v_in, ck_in, cv_in, g_in, l_in, d_in, r_in,
    att, rec,
    kf, vf, qf, kp, vp, wm, wq, wdq, wdr, wdt, kt, sc, ao, gd, ps, pr, gs, rr, ym, yd, xs, zs, ls,
    fr, fd, ro, rt, hq, ql,
    s_loc, s_hp, s_par, s_ring, s_fwd, s_wy, s_wp, s_wr, s_wf, s_qr, s_qfw, s_rsp, s_rs, s_ag, s_ag2,
    s_dag, s_dag2, s_dp, s_fr, s_oa, s_or, snd,
):
    z = lax.axis_index("z")
    x = lax.axis_index("x")
    c = lax.axis_index("c")
    y = lax.axis_index("y")
    p = 1 - c
    right = lax.rem(x + 1, 4)
    left = lax.rem(x + 3, 4)
    far = lax.rem(x + 2, 4)
    me = 2 * x + c
    head = lax.rem(z, 2)
    source = y == z // 2
    partner = (z, x, p, y)

    def at(start, size):
        return pl.ds(pl.multiple_of(start, size), size)

    mine = at(me * 64, 64)
    half = at(c * HALF, HALF)
    other = at(p * HALF, HALF)
    own = at(c * 64, 64)
    theirs = at(p * 64, 64)
    quarter = at(x * 128, 128)
    down_rows = at(c * 256, 256)
    down_piece = at(x * 128 + c * 64, 64)

    def got(ref, sem):
        remote(ref, ref, snd.at[0], sem, partner).wait_recv()

    loads = [
        local(k_in.at[:, half], kf.at[mine, :], s_loc.at[0]),
        local(v_in.at[:, half], vf.at[mine, :], s_loc.at[1]),
        local(q_in.at[:, half], qf.at[mine, :], s_loc.at[2]),
        local(r_in.at[:, at(y * 2 * HALF + c * HALF, HALF)], rt, s_loc.at[3]),
    ]
    for load in loads:
        load.start()

    @pl.when(c == 1)
    def _():
        local(k_in.at[:, :HALF], kp.at[own, :], s_hp.at[0, c]).start()
        local(v_in.at[:, :HALF], vp.at[own, :], s_hp.at[1, c]).start()

    @pl.when((c == 0) & (y == 0))
    def _():
        local(ck_in, kp.at[own, :], s_hp.at[0, c]).start()
        local(cv_in, vp.at[own, :], s_hp.at[1, c]).start()

    def full_weights(first, second):
        return [
            local(first.at[head], wm, s_wy.at[0]),
            local(second.at[head, quarter, :], wq.at[at(p * 128, 128), :], s_wy.at[1]),
            local(d_in.at[head, :, quarter], wdq, s_wy.at[2]),
            local(d_in.at[head, quarter, :], wdr, s_wy.at[3]),
        ]

    for core, (first, second) in enumerate(((g_in, l_in), (l_in, g_in))):

        @pl.when(source & (c == core))
        def _():
            for load in full_weights(first, second):
                load.start()

    barrier = pltpu.get_barrier_semaphore()
    peers = [partner]
    for step in range(1, 4):
        for core in range(2):
            peers.append((z, lax.rem(x + step, 4), core, y))
            peers.append((z, x, core, lax.rem(y + step, 4)))
    for peer in peers:
        pl.semaphore_signal(barrier, inc=1, device_id=peer, device_id_type=pl.DeviceIdType.MESH)
    pl.semaphore_wait(barrier, len(peers))

    for core, first in enumerate((g_in, l_in)):

        @pl.when(source & (c == core))
        def _():
            for step in (2, 1, 3):
                to = (z, x, c, lax.rem(y + step, 4))
                remote(
                    first.at[head, quarter, :], wm.at[quarter, :], snd.at[0], s_wy.at[0], to
                ).start()
                remote(
                    d_in.at[head, down_rows, quarter],
                    wdq.at[down_rows, :],
                    snd.at[0],
                    s_wy.at[1],
                    to,
                ).start()

    share = [
        remote(k_in.at[:, other], kf.at[mine, :], snd.at[1], s_par.at[0], partner),
        remote(v_in.at[:, other], vf.at[mine, :], snd.at[2], s_par.at[1], partner),
        remote(q_in.at[:, other], qf.at[mine, :], snd.at[3], s_par.at[2], partner),
    ]
    for copy in share:
        copy.start()

    def prior(ks, vs, to, index):
        return [
            remote(ks, kp.at[own, :], snd.at[index], s_hp.at[0, c], to),
            remote(vs, vp.at[own, :], snd.at[index + 1], s_hp.at[1, c], to),
        ]

    within = prior(k_in.at[:, :HALF], v_in.at[:, :HALF], partner, 4)
    cached = prior(ck_in, cv_in, partner, 4)
    halo = prior(k_in.at[:, HALF:], v_in.at[:, HALF:], (z, x, 0, lax.rem(y + 1, 4)), 25)

    @pl.when(c == 0)
    def _():
        for copy in within:
            copy.start()

    @pl.when((c == 1) & (y == 0))
    def _():
        for copy in cached:
            copy.start()

    def spread(src, dst, send, recv, first, size):
        for way, to in enumerate((right, left)):
            for core in range(2):
                remote(
                    src.at[:, core * HALF + first : core * HALF + first + size],
                    dst.at[mine, first : first + size],
                    send,
                    recv.at[way],
                    (z, to, core, y),
                ).start()

    for block in range(NBLK):
        for index, (src, dst) in enumerate(((k_in, kf), (v_in, vf))):
            spread(src, dst, snd.at[8 + index], s_ring.at[index, block], block * BLK, BLK)

    @pl.when(y < 3)
    def _():
        for copy in halo:
            copy.start()

    @pl.when(source)
    def _():
        for step in (2, 1, 3):
            to = (z, x, c, lax.rem(y + step, 4))
            remote(
                d_in.at[head, down_piece, :], wdr.at[own, :], snd.at[6], s_wy.at[2], to
            ).start()

    chips = (left, right)
    for block in range(NBLK):
        span = slice(block * BLK, (block + 1) * BLK)
        for index, dst in enumerate((kf, vf)):
            part = dst.at[at(chips[index] * 128, 128), span]
            got(part, s_ring.at[index, block, index])
            to = (z, chips[1 - index], c, y)
            remote(part, part, snd.at[14], s_fwd.at[index, block], to).start()

    wm_quarter = wm.at[quarter, :]
    weight_share = [
        remote(wm_quarter, wq.at[at(c * 128, 128), :], snd.at[11], s_wp.at[0], partner),
        remote(wdq.at[down_rows, :], wdq.at[down_rows, :], snd.at[12], s_wp.at[1], partner),
    ]

    @pl.when(jnp.logical_not(source))
    def _():
        got(wm_quarter, s_wy.at[0])
        got(wdq.at[down_rows, :], s_wy.at[1])
        for copy in weight_share:
            copy.start()
        for way, to in enumerate((right, left)):
            remote(wm_quarter, wm_quarter, snd.at[16], s_wr.at[way], (z, to, c, y)).start()

    spread(q_in, qf, snd.at[10], s_qr, 0, HALF)

    for load in loads:
        load.wait()
    for index, dst in enumerate((kp, vp)):
        for core in range(2):
            got(dst.at[core * 64 : (core + 1) * 64, :], s_hp.at[index, core])
    for index, dst in enumerate((kf, vf, qf)):
        got(dst.at[at((2 * x + p) * 64, 64), :], s_par.at[index])

    for block in range(NBLK):
        span = slice(block * BLK, (block + 1) * BLK)
        kt[block * BLK : (block + 1) * BLK, :] = kp[:, span].T
        kt[HALF + block * BLK : HALF + (block + 1) * BLK, :] = kf[quarter, span].T

    row_at = lax.broadcasted_iota(jnp.int32, (BLK, BLK), 0)
    col_at = lax.broadcasted_iota(jnp.int32, (BLK, BLK), 1)

    def attend(block):
        first = block * BLK
        asked = qf[quarter, first : first + BLK]
        top = jnp.full((1, BLK), -jnp.inf, F32)
        for part in range(5):
            key = first + part * BLK
            scores = dot(kt[key : key + BLK, :], asked) * SCALE
            if part == 0:
                scores = jnp.where(row_at > col_at, scores, -jnp.inf)
            if part == 4:
                scores = jnp.where(row_at <= col_at, scores, -jnp.inf)
            sc[part * BLK : (part + 1) * BLK, :] = scores
            top = jnp.maximum(top, jnp.max(scores, axis=0, keepdims=True))
        total = jnp.zeros((1, BLK), F32)
        blend = jnp.zeros((128, BLK), F32)
        for part in range(5):
            key = first + part * BLK
            raised = jnp.exp2(sc[part * BLK : (part + 1) * BLK, :] - top)
            total = total + jnp.sum(raised, axis=0, keepdims=True)
            if key < HALF:
                held = vp[:, key : key + BLK]
            else:
                held = vf[quarter, key - HALF : key - HALF + BLK]
            blend = blend + dot(held, raised.astype(BF16))
        ao[:, first : first + BLK] = (blend / total).astype(BF16)

    attend(0)

    for core, (first, second) in enumerate(((g_in, l_in), (l_in, g_in))):

        @pl.when(source & (c == core))
        def _():
            for load in full_weights(first, second):
                load.wait()

    @pl.when(jnp.logical_not(source))
    def _():
        got(wq.at[at(p * 128, 128), :], s_wp.at[0])
        got(wdq.at[at(p * 256, 256), :], s_wp.at[1])

    wq[at(c * 128, 128), :] = wm[quarter, :]
    for block in range(4):
        wdt[:, block * 128 : (block + 1) * 128] = wdq[block * 128 : (block + 1) * 128, :].T

    gd[...] = jnp.zeros_like(gd)
    for block in range(NBLK):
        span = slice(block * BLK, (block + 1) * BLK)
        for index, dst in enumerate((kf, vf)):
            got(dst.at[at(chips[1 - index] * 128, 128), span], s_ring.at[index, block, 1 - index])
            got(dst.at[at(far * 128, 128), span], s_fwd.at[index, block])
        keys = kf[:, span]
        rate = rt[pl.ds(z, 1), span]
        target = (-(vf[:, span].astype(F32) * rate)).astype(BF16)
        pre_gate = dot(wq[0:128, :], keys)
        pre_lift = dot(wq[128:256, :], keys)
        back = dot(wdt[...], target)
        sig = 1.0 / (1.0 + jnp.exp(-pre_gate))
        silu = pre_gate * sig
        hidden = (silu * pre_lift).astype(BF16)
        back_lift = (back * silu).astype(BF16)
        back_gate = (back * pre_lift * sig * (1.0 + pre_gate * (1.0 - sig))).astype(BF16)
        gd[0:128, :] += dot_t(back_gate, keys)
        gd[128:256, :] += dot_t(back_lift, keys)
        gd[256:384, :] += dot_t(hidden, target)

    main, down = slice(0, 128), slice(128, 256)
    ps[main, :] = gd[at(p * 128, 128), :].astype(BF16)
    remote(ps.at[main, :], pr.at[main, :], snd.at[15], s_rsp.at[0], partner).start()

    @pl.when(c == 0)
    def _():
        ps[down, :] = gd[256:384, :].astype(BF16)
        remote(ps.at[down, :], pr.at[down, :], snd.at[28], s_rsp.at[1], partner).start()

    attend(1)

    def pair_and_send(index, span, first, size, low):
        got(pr.at[span, :], s_rsp.at[index])
        rows = slice(low, low + size)
        for owner in range(4):
            begin_at = span.start + owner * size
            both = gd[at(first + owner * size, size), :] + pr[
                begin_at : begin_at + size, :
            ].astype(F32)
            gs[owner, rows, :] = both.astype(BF16)
            ls[begin_at : begin_at + size, :] = both
        for step in (2, 1, 3):
            owner = lax.rem(y + step, 4)
            remote(
                gs.at[owner, rows, :],
                rr.at[y, rows, :],
                snd.at[17 + 10 * index],
                s_rs.at[index],
                (z, x, c, owner),
            ).start()

    def summed(index, span, size, low):
        rows = slice(low, low + size)
        got(rr.at[0:3, rows, :], s_rs.at[index])
        whole = ls[at(span.start + y * size, size), :]
        for step in range(1, 4):
            whole = whole + rr[lax.rem(y + step, 4), rows, :].astype(F32)
        return whole.astype(BF16)

    pair_and_send(0, main, c * 128, 32, 0)

    @pl.when(c == 1)
    def _():
        pair_and_send(1, down, 256, 32, 32)

    attend(2)
    attend(3)
    local(ao.at[own, :], att.at[:, half], s_loc.at[4]).start()
    give = remote(ao.at[theirs, :], att.at[:, half], snd.at[23], s_oa, partner)
    give.start()
    ym[4 * x + y] = summed(0, main, 32, 0)

    def gather(ref, index, ways, recv_low, recv_high, send):
        for step in (2, 1, 3):
            in_y = (z, x, c, lax.rem(y + step, 4))
            in_x = (z, lax.rem(x + step, 4), c, y)
            low, high = ref.at[index, :, 0:256], ref.at[index, :, 256:512]
            to_low, to_high = (in_y, in_x) if ways == 0 else (in_x, in_y)
            remote(low, low, send, recv_low(step), to_low).start()
            remote(high, high, send, recv_high(step), to_high).start()

    def gather_first(ref, index, first, send):
        gather(ref, index, 0, lambda n: first.at[0, n], lambda n: first.at[1, n], send)

    def gather_rest(ref, index, second, send):
        gather(ref, index, 1, lambda n: second, lambda n: second, send)

    def relay(ref, index_of, first, second, send):
        low, high = slice(0, 256), slice(256, 512)
        for step in (1, 3, 2):
            across = index_of(x, lax.rem(y + 4 - step, 4))
            part = ref.at[across, :, low]
            got(part, first.at[0, step])
            for hop in (2, 1, 3):
                to = (z, lax.rem(x + hop, 4), c, y)
                remote(part, part, send, second, to).start()
            along = index_of(lax.rem(x + 4 - step, 4), y)
            part = ref.at[along, :, high]
            got(part, first.at[1, step])
            for hop in (2, 1, 3):
                to = (z, x, c, lax.rem(y + hop, 4))
                remote(part, part, send, second, to).start()

    def main_at(xx, yy):
        return 4 * xx + yy

    place = main_at(x, y)
    gather_first(ym, place, s_ag, snd.at[18])
    gather_rest(ym, place, s_ag2, snd.at[18])

    @pl.when(c == 1)
    def _():
        yd[place] = summed(1, down, 32, 32)
        gather_first(yd, place, s_dag, snd.at[19])

    relay(ym, main_at, s_ag, s_ag2, snd.at[18])

    @pl.when(c == 1)
    def _():
        gather_rest(yd, place, s_dag2, snd.at[19])
        relay(yd, main_at, s_dag, s_dag2, snd.at[19])

    @pl.when(jnp.logical_not(source))
    def _():
        for way in range(2):
            got(wm_quarter, s_wr.at[way])
        for index in range(2):
            part = wm.at[at(chips[index] * 128 + index * 64, 64), :]
            to = (z, chips[1 - index], c, y)
            remote(part, part, snd.at[21], s_wf.at[index], to).start()
        got(wdr.at[own, :], s_wy.at[2])
        remote(wdr.at[own, :], wdr.at[own, :], snd.at[22], s_wp.at[2], partner).start()

    for way in range(2):
        rows = at(chips[way] * 128, 128)
        got(qf.at[rows, :], s_qr.at[way])
        part = qf.at[rows, way * 512 : way * 512 + 512]
        remote(part, part, snd.at[7], s_qfw.at[way], (z, chips[1 - way], c, y)).start()

    def begin(rounded):
        wide = rounded.astype(F32)
        norm = jnp.sqrt(jnp.sum(jnp.square(wide), keepdims=True) + EPS)
        return (wide / norm).astype(BF16)

    def sweep():
        zs[...] = dot_t(xs[...], xs[...]).astype(BF16)
        fd[...] = dot(zs[...], xs[...]).astype(BF16)
        xs[...] = (
            COEF_A * xs[...].astype(F32)
            + COEF_B * fd[...].astype(F32)
            + COEF_C * dot(zs[...], fd[...])
        ).astype(BF16)

    def fresh(weight, turned):
        initial = weight.astype(F32)
        moved = initial - turned.astype(F32)
        wanted = jnp.sqrt(jnp.mean(jnp.square(initial), axis=-1, keepdims=True) + EPS)
        present = jnp.sqrt(jnp.mean(jnp.square(moved), axis=-1, keepdims=True) + EPS)
        return (moved * (wanted / present)).astype(BF16)

    got(ym.at[0:12], s_ag2)
    xs[...] = begin(ym[...].reshape(512, 512))
    sweep()
    sweep()

    @pl.when(jnp.logical_not(source))
    def _():
        for index in range(2):
            got(wm.at[at(far * 128 + index * 64, 64), :], s_wf.at[index])

    lends = []
    for index in range(2):
        rows = slice(index * 256, index * 256 + 256)
        fr[c, rows, :] = fresh(wm[rows, :], xs[rows, :])
        part = fr.at[c, rows, :]
        lends.append(remote(part, part, snd.at[13 + 16 * index], s_fr.at[index], partner))
        lends[index].start()

    @pl.when(jnp.logical_not(source))
    def _():
        got(wdr.at[theirs, :], s_wp.at[2])

    lend_down = remote(fd.at[0:128, :], wdt, snd.at[20], s_dp, partner)

    @pl.when(c == 1)
    def _():
        got(yd.at[0:12], s_dag2)
        xs[...] = begin(yd[...].reshape(512, 512))
        sweep()
        zs[...] = dot_t(xs[...], xs[...]).astype(BF16)
        side = xs[:, quarter]
        lifted = dot(zs[...], side).astype(BF16)
        turned = (
            COEF_A * side.astype(F32) + COEF_B * lifted.astype(F32) + COEF_C * dot(zs[...], lifted)
        ).astype(BF16)
        new = fresh(wdr[...], turned.T)
        fd[0:128, :] = new
        wdt[...] = new
        lend_down.start()

    for way in range(2):
        got(qf.at[at(far * 128, 128), way * 512 : way * 512 + 512], s_qfw.at[way])
    def lent():
        for index in range(2):
            got(fr.at[p, index * 256 : index * 256 + 256, :], s_fr.at[index])

    def hide(block, query_lift):
        span = slice(block * BLK, (block + 1) * BLK)
        query_gate = dot(fr[0], qf[:, span])
        return (query_gate / (1.0 + jnp.exp(-query_gate)) * query_lift).astype(BF16)

    def settle(block, hidden):
        span = slice(block * BLK, (block + 1) * BLK)
        ro[:, span] = dot(wdt[...], hidden).astype(BF16)
        here = at(c * HALF + block * BLK, BLK)
        remote(ro.at[theirs, span], rec.at[:, here], snd.at[24], s_or, partner).start()
        local(ro.at[own, span], rec.at[:, here], s_loc.at[5 + block]).start()

    @pl.when(c == 0)
    def _():
        lent()
        for block in range(NBLK):
            span = slice(block * BLK, (block + 1) * BLK)
            hq[:, span] = hide(block, dot(fr[1], qf[:, span]))
        got(wdt, s_dp)
        for block in range(NBLK):
            settle(block, hq[:, block * BLK : (block + 1) * BLK])

    @pl.when(c == 1)
    def _():
        for block in range(NBLK):
            span = slice(block * BLK, (block + 1) * BLK)
            ql[:, span] = dot(fr[1], qf[:, span])
        lent()
        for block in range(NBLK):
            settle(block, hide(block, ql[:, block * BLK : (block + 1) * BLK]))

    def drain(ref, index):
        remote(ref, ref, snd.at[index], s_or, partner).wait_send()

    for block in range(NBLK):
        span = slice(block * BLK, (block + 1) * BLK)
        local(ro.at[own, span], ro.at[own, span], s_loc.at[5 + block]).wait()
    local(ao.at[own, :], att.at[:, half], s_loc.at[4]).wait()
    give.wait_send()
    got(ao.at[own, :], s_oa)
    for copy in lends:
        copy.wait_send()
    for copy in share:
        copy.wait_send()

    @pl.when(c == 0)
    def _():
        for copy in within:
            copy.wait_send()

    @pl.when((c == 1) & (y == 0))
    def _():
        for copy in cached:
            copy.wait_send()

    @pl.when(y < 3)
    def _():
        for copy in halo:
            copy.wait_send()

    @pl.when(source)
    def _():
        drain(kf.at[0:288, :], 0)
        drain(wm.at[0:192, :], 6)

    for index in range(2):
        drain(kf.at[0:256, :], 8 + index)
    drain(kf.at[0:256, :], 14)
    drain(kf.at[0:256, :], 10)
    drain(kf.at[0:128, :], 7)

    @pl.when(jnp.logical_not(source))
    def _():
        for copy in weight_share:
            copy.wait_send()
        drain(wm.at[0:256, :], 16)
        drain(wm.at[0:128, :], 21)
        drain(wdr.at[own, :], 22)

    drain(pr.at[main, :], 15)
    drain(rr.at[0:3, 0:32], 17)
    drain(ym.at[0:15], 18)

    @pl.when(c == 0)
    def _():
        drain(pr.at[down, :], 28)

    @pl.when(c == 1)
    def _():
        drain(rr.at[0:3, 32:64], 27)
        drain(yd.at[0:15], 19)
        lend_down.wait_send()

    drain(ro.at[0:64, :], 24)
    got(ro.at[0:64, :], s_or)


def write_out(att, rec, att_out, rec_out, sem):
    copies = [local(att, att_out, sem.at[0]), local(rec, rec_out, sem.at[1])]
    for copy in copies:
        copy.start()
    for copy in copies:
        copy.wait()


def per_device(*arrays):
    any_spec = pl.BlockSpec(memory_space=pl.ANY)
    out = pltpu.VMEM((64, 2 * HALF), BF16)
    arrays = [pltpu.with_memory_space_constraint(a, pltpu.HBM) for a in arrays]
    vmem = pltpu.VMEM
    dma = pltpu.SemaphoreType.DMA
    held = pl.pallas_call(
        kernel,
        out_shape=(out, out),
        in_specs=[any_spec] * 9,
        out_specs=(any_spec, any_spec),
        scratch_shapes=[
            vmem((512, HALF), BF16),
            vmem((512, HALF), BF16),
            vmem((512, HALF), BF16),
            vmem((128, HALF), BF16),
            vmem((128, HALF), BF16),
            vmem((512, 512), BF16),
            vmem((256, 512), BF16),
            vmem((512, 128), BF16),
            vmem((128, 512), BF16),
            vmem((128, 512), BF16),
            vmem((2 * HALF, 128), BF16),
            vmem((5 * BLK, BLK), F32),
            vmem((128, HALF), BF16),
            vmem((384, 512), F32),
            vmem((256, 512), BF16),
            vmem((256, 512), BF16),
            vmem((4, 64, 512), BF16),
            vmem((4, 64, 512), BF16),
            vmem((16, 32, 512), BF16),
            vmem((16, 32, 512), BF16),
            vmem((512, 512), BF16),
            vmem((512, 512), BF16),
            vmem((256, 512), F32),
            vmem((2, 512, 512), BF16),
            vmem((512, 512), BF16),
            vmem((128, HALF), BF16),
            vmem((8, HALF), F32),
            vmem((512, HALF), BF16),
            vmem((512, HALF), F32),
            dma((9,)),
            dma((2, 2)),
            dma((3,)),
            dma((2, NBLK, 2)),
            dma((2, NBLK)),
            dma((4,)),
            dma((3,)),
            dma((2,)),
            dma((2,)),
            dma((2,)),
            dma((2,)),
            dma((2,)),
            dma((2,)),
            dma((2, 4)),
            dma(()),
            dma((2, 4)),
            dma(()),
            dma(()),
            dma((2,)),
            dma(()),
            dma(()),
            dma((30,)),
        ],
        compiler_params=pltpu.CompilerParams(
            collective_id=0, has_side_effects=True, vmem_limit_bytes=48000000
        ),
        name="plane",
    )(*arrays)
    return pl.pallas_call(
        write_out,
        out_shape=(pltpu.HBM((64, 2 * HALF), BF16),) * 2,
        in_specs=[pl.BlockSpec(memory_space=vmem)] * 2,
        out_specs=(pl.BlockSpec(memory_space=pltpu.HBM),) * 2,
        scratch_shapes=[dma((2,))],
        name="write_out",
    )(*[pltpu.with_memory_space_constraint(a, pltpu.VMEM) for a in held])


def solution(mesh):
    split = Mesh(mesh.devices.reshape(8, 4, 2, 4), ("z", "x", "c", "y"))
    tokens = P(WIDE, "y")
    heads = P("y", None, None)
    return jax.shard_map(
        per_device,
        mesh=split,
        in_specs=(tokens, tokens, tokens, P(WIDE), P(WIDE), heads, heads, heads, P()),
        out_specs=(tokens, tokens),
        check_vma=False,
    )
```

```python
import functools
import math

import jax
import jax.numpy as jnp
from jax import lax
from jax.experimental import pallas as pl
from jax.experimental.pallas import tpu as pltpu
from jax.sharding import Mesh
from jax.sharding import PartitionSpec as P

WIDE = ("z", "x", "c")
EPS = 1e-06
COEF_A = 3.4445
COEF_B = -4.775
COEF_C = 2.0315
HALF = 1024
BLK = 256
NBLK = HALF // BLK
SCALE = math.log2(math.e) / math.sqrt(128)
F32 = jnp.float32
BF16 = jnp.bfloat16


def dot(a, b):
    return lax.dot_general(a, b, (((1,), (0,)), ((), ())), preferred_element_type=F32)


def dot_t(a, b):
    return lax.dot_general(a, b, (((1,), (1,)), ((), ())), preferred_element_type=F32)


def local(src, dst, sem):
    return pltpu.make_async_copy(src, dst, sem)


def remote(src, dst, send, recv, device):
    return pltpu.make_async_remote_copy(
        src_ref=src,
        dst_ref=dst,
        send_sem=send,
        recv_sem=recv,
        device_id=device,
        device_id_type=pl.DeviceIdType.MESH,
    )


def kernel(
    q_in, k_in, v_in, ck_in, cv_in, g_in, l_in, d_in, r_in,
    att, rec,
    kf, vf, qf, kp, vp, wm, wq, wdq, wdr, wdt, kt, sc, ao, gd, ps, pr, gs, rr, ym, yd, xs, zs, ls,
    fr, fd, ro, rt, hq, ql,
    s_loc, s_hp, s_par, s_ring, s_fwd, s_wy, s_wp, s_wr, s_wf, s_qr, s_qfw, s_rsp, s_rs, s_ag, s_ag2,
    s_dag, s_dag2, s_dp, s_fr, s_oa, s_or, snd,
):
    z = lax.axis_index("z")
    x = lax.axis_index("x")
    c = lax.axis_index("c")
    y = lax.axis_index("y")
    p = 1 - c
    right = lax.rem(x + 1, 4)
    left = lax.rem(x + 3, 4)
    far = lax.rem(x + 2, 4)
    me = 2 * x + c
    head = lax.rem(z, 2)
    source = y == z // 2
    partner = (z, x, p, y)

    def at(start, size):
        return pl.ds(pl.multiple_of(start, size), size)

    mine = at(me * 64, 64)
    half = at(c * HALF, HALF)
    other = at(p * HALF, HALF)
    own = at(c * 64, 64)
    theirs = at(p * 64, 64)
    quarter = at(x * 128, 128)
    down_rows = at(c * 256, 256)
    down_piece = at(x * 128 + c * 64, 64)

    def got(ref, sem):
        remote(ref, ref, snd.at[0], sem, partner).wait_recv()

    loads = [
        local(k_in.at[:, half], kf.at[mine, :], s_loc.at[0]),
        local(v_in.at[:, half], vf.at[mine, :], s_loc.at[1]),
        local(q_in.at[:, half], qf.at[mine, :], s_loc.at[2]),
        local(r_in.at[:, at(y * 2 * HALF + c * HALF, HALF)], rt, s_loc.at[3]),
    ]
    for load in loads:
        load.start()

    @pl.when(c == 1)
    def _():
        local(k_in.at[:, :HALF], kp.at[own, :], s_hp.at[0, c]).start()
        local(v_in.at[:, :HALF], vp.at[own, :], s_hp.at[1, c]).start()

    @pl.when((c == 0) & (y == 0))
    def _():
        local(ck_in, kp.at[own, :], s_hp.at[0, c]).start()
        local(cv_in, vp.at[own, :], s_hp.at[1, c]).start()

    def full_weights(first, second):
        return [
            local(first.at[head], wm, s_wy.at[0]),
            local(second.at[head, quarter, :], wq.at[at(p * 128, 128), :], s_wy.at[1]),
            local(d_in.at[head, :, quarter], wdq, s_wy.at[2]),
            local(d_in.at[head, quarter, :], wdr, s_wy.at[3]),
        ]

    for core, (first, second) in enumerate(((g_in, l_in), (l_in, g_in))):

        @pl.when(source & (c == core))
        def _():
            for load in full_weights(first, second):
                load.start()

    barrier = pltpu.get_barrier_semaphore()
    peers = [partner]
    for step in range(1, 4):
        for core in range(2):
            peers.append((z, lax.rem(x + step, 4), core, y))
            peers.append((z, x, core, lax.rem(y + step, 4)))
    for peer in peers:
        pl.semaphore_signal(barrier, inc=1, device_id=peer, device_id_type=pl.DeviceIdType.MESH)
    pl.semaphore_wait(barrier, len(peers))

    for core, first in enumerate((g_in, l_in)):

        @pl.when(source & (c == core))
        def _():
            for step in (2, 1, 3):
                to = (z, x, c, lax.rem(y + step, 4))
                remote(
                    first.at[head, quarter, :], wm.at[quarter, :], snd.at[0], s_wy.at[0], to
                ).start()
                remote(
                    d_in.at[head, down_rows, quarter],
                    wdq.at[down_rows, :],
                    snd.at[0],
                    s_wy.at[1],
                    to,
                ).start()

    share = [
        remote(k_in.at[:, other], kf.at[mine, :], snd.at[1], s_par.at[0], partner),
        remote(v_in.at[:, other], vf.at[mine, :], snd.at[2], s_par.at[1], partner),
        remote(q_in.at[:, other], qf.at[mine, :], snd.at[3], s_par.at[2], partner),
    ]
    for copy in share:
        copy.start()

    def prior(ks, vs, to, index):
        return [
            remote(ks, kp.at[own, :], snd.at[index], s_hp.at[0, c], to),
            remote(vs, vp.at[own, :], snd.at[index + 1], s_hp.at[1, c], to),
        ]

    within = prior(k_in.at[:, :HALF], v_in.at[:, :HALF], partner, 4)
    cached = prior(ck_in, cv_in, partner, 4)
    halo = prior(k_in.at[:, HALF:], v_in.at[:, HALF:], (z, x, 0, lax.rem(y + 1, 4)), 25)

    @pl.when(c == 0)
    def _():
        for copy in within:
            copy.start()

    @pl.when((c == 1) & (y == 0))
    def _():
        for copy in cached:
            copy.start()

    def spread(src, dst, send, recv, first, size):
        for way, to in enumerate((right, left)):
            for core in range(2):
                remote(
                    src.at[:, core * HALF + first : core * HALF + first + size],
                    dst.at[mine, first : first + size],
                    send,
                    recv.at[way],
                    (z, to, core, y),
                ).start()

    for block in range(NBLK):
        for index, (src, dst) in enumerate(((k_in, kf), (v_in, vf))):
            spread(src, dst, snd.at[8 + index], s_ring.at[index, block], block * BLK, BLK)

    @pl.when(y < 3)
    def _():
        for copy in halo:
            copy.start()

    @pl.when(source)
    def _():
        for step in (2, 1, 3):
            to = (z, x, c, lax.rem(y + step, 4))
            remote(
                d_in.at[head, down_piece, :], wdr.at[own, :], snd.at[6], s_wy.at[2], to
            ).start()

    chips = (left, right)
    for block in range(NBLK):
        span = slice(block * BLK, (block + 1) * BLK)
        for index, dst in enumerate((kf, vf)):
            part = dst.at[at(chips[index] * 128, 128), span]
            got(part, s_ring.at[index, block, index])
            to = (z, chips[1 - index], c, y)
            remote(part, part, snd.at[14], s_fwd.at[index, block], to).start()

    wm_quarter = wm.at[quarter, :]
    weight_share = [
        remote(wm_quarter, wq.at[at(c * 128, 128), :], snd.at[11], s_wp.at[0], partner),
        remote(wdq.at[down_rows, :], wdq.at[down_rows, :], snd.at[12], s_wp.at[1], partner),
    ]

    @pl.when(jnp.logical_not(source))
    def _():
        got(wm_quarter, s_wy.at[0])
        got(wdq.at[down_rows, :], s_wy.at[1])
        for copy in weight_share:
            copy.start()
        for way, to in enumerate((right, left)):
            remote(wm_quarter, wm_quarter, snd.at[16], s_wr.at[way], (z, to, c, y)).start()

    spread(q_in, qf, snd.at[10], s_qr, 0, HALF)

    for load in loads:
        load.wait()
    for index, dst in enumerate((kf, vf, qf)):
        got(dst.at[at((2 * x + p) * 64, 64), :], s_par.at[index])

    row_at = lax.broadcasted_iota(jnp.int32, (BLK, BLK), 0)
    col_at = lax.broadcasted_iota(jnp.int32, (BLK, BLK), 1)

    def attend(block):
        first = block * BLK
        asked = qf[quarter, first : first + BLK]
        top = jnp.full((1, BLK), -jnp.inf, F32)
        for part in range(5):
            key = first + part * BLK
            scores = dot(kt[key : key + BLK, :], asked) * SCALE
            if part == 0:
                scores = jnp.where(row_at > col_at, scores, -jnp.inf)
            if part == 4:
                scores = jnp.where(row_at <= col_at, scores, -jnp.inf)
            sc[part * BLK : (part + 1) * BLK, :] = scores
            top = jnp.maximum(top, jnp.max(scores, axis=0, keepdims=True))
        total = jnp.zeros((1, BLK), F32)
        blend = jnp.zeros((128, BLK), F32)
        for part in range(5):
            key = first + part * BLK
            raised = jnp.exp2(sc[part * BLK : (part + 1) * BLK, :] - top)
            total = total + jnp.sum(raised, axis=0, keepdims=True)
            if key < HALF:
                held = vp[:, key : key + BLK]
            else:
                held = vf[quarter, key - HALF : key - HALF + BLK]
            blend = blend + dot(held, raised.astype(BF16))
        ao[:, first : first + BLK] = (blend / total).astype(BF16)

    for core, (first, second) in enumerate(((g_in, l_in), (l_in, g_in))):

        @pl.when(source & (c == core))
        def _():
            for load in full_weights(first, second):
                load.wait()

    @pl.when(jnp.logical_not(source))
    def _():
        got(wq.at[at(p * 128, 128), :], s_wp.at[0])
        got(wdq.at[at(p * 256, 256), :], s_wp.at[1])

    wq[at(c * 128, 128), :] = wm[quarter, :]
    for block in range(4):
        wdt[:, block * 128 : (block + 1) * 128] = wdq[block * 128 : (block + 1) * 128, :].T

    gd[...] = jnp.zeros_like(gd)
    for block in range(NBLK):
        span = slice(block * BLK, (block + 1) * BLK)
        for index, dst in enumerate((kf, vf)):
            got(dst.at[at(chips[1 - index] * 128, 128), span], s_ring.at[index, block, 1 - index])
            got(dst.at[at(far * 128, 128), span], s_fwd.at[index, block])
        keys = kf[:, span]
        rate = rt[pl.ds(z, 1), span]
        target = (-(vf[:, span].astype(F32) * rate)).astype(BF16)
        pre_gate = dot(wq[0:128, :], keys)
        pre_lift = dot(wq[128:256, :], keys)
        back = dot(wdt[...], target)
        sig = 1.0 / (1.0 + jnp.exp(-pre_gate))
        silu = pre_gate * sig
        hidden = (silu * pre_lift).astype(BF16)
        back_lift = (back * silu).astype(BF16)
        back_gate = (back * pre_lift * sig * (1.0 + pre_gate * (1.0 - sig))).astype(BF16)
        gd[0:128, :] += dot_t(back_gate, keys)
        gd[128:256, :] += dot_t(back_lift, keys)
        gd[256:384, :] += dot_t(hidden, target)

    main, down = slice(0, 128), slice(128, 256)
    ps[main, :] = gd[at(p * 128, 128), :].astype(BF16)
    remote(ps.at[main, :], pr.at[main, :], snd.at[15], s_rsp.at[0], partner).start()

    @pl.when(c == 0)
    def _():
        ps[down, :] = gd[256:384, :].astype(BF16)
        remote(ps.at[down, :], pr.at[down, :], snd.at[28], s_rsp.at[1], partner).start()


    def pair_and_send(index, span, first, size, low):
        got(pr.at[span, :], s_rsp.at[index])
        rows = slice(low, low + size)
        for owner in range(4):
            begin_at = span.start + owner * size
            both = gd[at(first + owner * size, size), :] + pr[
                begin_at : begin_at + size, :
            ].astype(F32)
            gs[owner, rows, :] = both.astype(BF16)
            ls[begin_at : begin_at + size, :] = both
        for step in (2, 1, 3):
            owner = lax.rem(y + step, 4)
            remote(
                gs.at[owner, rows, :],
                rr.at[y, rows, :],
                snd.at[17 + 10 * index],
                s_rs.at[index],
                (z, x, c, owner),
            ).start()

    def summed(index, span, size, low):
        rows = slice(low, low + size)
        got(rr.at[0:3, rows, :], s_rs.at[index])
        whole = ls[at(span.start + y * size, size), :]
        for step in range(1, 4):
            whole = whole + rr[lax.rem(y + step, 4), rows, :].astype(F32)
        return whole.astype(BF16)

    pair_and_send(0, main, c * 128, 32, 0)

    @pl.when(c == 1)
    def _():
        pair_and_send(1, down, 256, 32, 32)

    for index, dst in enumerate((kp, vp)):
        for core in range(2):
            got(dst.at[core * 64 : (core + 1) * 64, :], s_hp.at[index, core])
    for block in range(NBLK):
        span = slice(block * BLK, (block + 1) * BLK)
        kt[block * BLK : (block + 1) * BLK, :] = kp[:, span].T
        kt[HALF + block * BLK : HALF + (block + 1) * BLK, :] = kf[quarter, span].T

    attend(0)
    attend(1)
    attend(2)
    attend(3)
    local(ao.at[own, :], att.at[:, half], s_loc.at[4]).start()
    give = remote(ao.at[theirs, :], att.at[:, half], snd.at[23], s_oa, partner)
    give.start()
    ym[4 * x + y] = summed(0, main, 32, 0)

    def gather(ref, index, ways, recv_low, recv_high, send):
        for step in (2, 1, 3):
            in_y = (z, x, c, lax.rem(y + step, 4))
            in_x = (z, lax.rem(x + step, 4), c, y)
            low, high = ref.at[index, :, 0:256], ref.at[index, :, 256:512]
            to_low, to_high = (in_y, in_x) if ways == 0 else (in_x, in_y)
            remote(low, low, send, recv_low(step), to_low).start()
            remote(high, high, send, recv_high(step), to_high).start()

    def gather_first(ref, index, first, send):
        gather(ref, index, 0, lambda n: first.at[0, n], lambda n: first.at[1, n], send)

    def gather_rest(ref, index, second, send):
        gather(ref, index, 1, lambda n: second, lambda n: second, send)

    def relay(ref, index_of, first, second, send):
        low, high = slice(0, 256), slice(256, 512)
        for step in (1, 3, 2):
            across = index_of(x, lax.rem(y + 4 - step, 4))
            part = ref.at[across, :, low]
            got(part, first.at[0, step])
            for hop in (2, 1, 3):
                to = (z, lax.rem(x + hop, 4), c, y)
                remote(part, part, send, second, to).start()
            along = index_of(lax.rem(x + 4 - step, 4), y)
            part = ref.at[along, :, high]
            got(part, first.at[1, step])
            for hop in (2, 1, 3):
                to = (z, x, c, lax.rem(y + hop, 4))
                remote(part, part, send, second, to).start()

    def main_at(xx, yy):
        return 4 * xx + yy

    place = main_at(x, y)
    gather_first(ym, place, s_ag, snd.at[18])
    gather_rest(ym, place, s_ag2, snd.at[18])

    @pl.when(c == 1)
    def _():
        yd[place] = summed(1, down, 32, 32)
        gather_first(yd, place, s_dag, snd.at[19])

    relay(ym, main_at, s_ag, s_ag2, snd.at[18])

    @pl.when(c == 1)
    def _():
        gather_rest(yd, place, s_dag2, snd.at[19])
        relay(yd, main_at, s_dag, s_dag2, snd.at[19])

    @pl.when(jnp.logical_not(source))
    def _():
        for way in range(2):
            got(wm_quarter, s_wr.at[way])
        for index in range(2):
            part = wm.at[at(chips[index] * 128 + index * 64, 64), :]
            to = (z, chips[1 - index], c, y)
            remote(part, part, snd.at[21], s_wf.at[index], to).start()
        got(wdr.at[own, :], s_wy.at[2])
        remote(wdr.at[own, :], wdr.at[own, :], snd.at[22], s_wp.at[2], partner).start()

    for way in range(2):
        rows = at(chips[way] * 128, 128)
        got(qf.at[rows, :], s_qr.at[way])
        part = qf.at[rows, way * 512 : way * 512 + 512]
        remote(part, part, snd.at[7], s_qfw.at[way], (z, chips[1 - way], c, y)).start()

    def begin(rounded):
        wide = rounded.astype(F32)
        norm = jnp.sqrt(jnp.sum(jnp.square(wide), keepdims=True) + EPS)
        return (wide / norm).astype(BF16)

    def sweep():
        zs[...] = dot_t(xs[...], xs[...]).astype(BF16)
        fd[...] = dot(zs[...], xs[...]).astype(BF16)
        xs[...] = (
            COEF_A * xs[...].astype(F32)
            + COEF_B * fd[...].astype(F32)
            + COEF_C * dot(zs[...], fd[...])
        ).astype(BF16)

    def fresh(weight, turned):
        initial = weight.astype(F32)
        moved = initial - turned.astype(F32)
        wanted = jnp.sqrt(jnp.mean(jnp.square(initial), axis=-1, keepdims=True) + EPS)
        present = jnp.sqrt(jnp.mean(jnp.square(moved), axis=-1, keepdims=True) + EPS)
        return (moved * (wanted / present)).astype(BF16)

    got(ym.at[0:12], s_ag2)
    xs[...] = begin(ym[...].reshape(512, 512))
    sweep()
    sweep()

    @pl.when(jnp.logical_not(source))
    def _():
        for index in range(2):
            got(wm.at[at(far * 128 + index * 64, 64), :], s_wf.at[index])

    lends = []
    for index in range(2):
        rows = slice(index * 256, index * 256 + 256)
        fr[c, rows, :] = fresh(wm[rows, :], xs[rows, :])
        part = fr.at[c, rows, :]
        lends.append(remote(part, part, snd.at[13 + 16 * index], s_fr.at[index], partner))
        lends[index].start()

    @pl.when(jnp.logical_not(source))
    def _():
        got(wdr.at[theirs, :], s_wp.at[2])

    lend_down = remote(fd.at[0:128, :], wdt, snd.at[20], s_dp, partner)

    @pl.when(c == 1)
    def _():
        got(yd.at[0:12], s_dag2)
        xs[...] = begin(yd[...].reshape(512, 512))
        sweep()
        zs[...] = dot_t(xs[...], xs[...]).astype(BF16)
        side = xs[:, quarter]
        lifted = dot(zs[...], side).astype(BF16)
        turned = (
            COEF_A * side.astype(F32) + COEF_B * lifted.astype(F32) + COEF_C * dot(zs[...], lifted)
        ).astype(BF16)
        new = fresh(wdr[...], turned.T)
        fd[0:128, :] = new
        wdt[...] = new
        lend_down.start()

    for way in range(2):
        got(qf.at[at(far * 128, 128), way * 512 : way * 512 + 512], s_qfw.at[way])
    def lent():
        for index in range(2):
            got(fr.at[p, index * 256 : index * 256 + 256, :], s_fr.at[index])

    def hide(block, query_lift):
        span = slice(block * BLK, (block + 1) * BLK)
        query_gate = dot(fr[0], qf[:, span])
        return (query_gate / (1.0 + jnp.exp(-query_gate)) * query_lift).astype(BF16)

    def settle(block, hidden):
        span = slice(block * BLK, (block + 1) * BLK)
        ro[:, span] = dot(wdt[...], hidden).astype(BF16)
        here = at(c * HALF + block * BLK, BLK)
        remote(ro.at[theirs, span], rec.at[:, here], snd.at[24], s_or, partner).start()
        local(ro.at[own, span], rec.at[:, here], s_loc.at[5 + block]).start()

    @pl.when(c == 0)
    def _():
        lent()
        for block in range(NBLK):
            span = slice(block * BLK, (block + 1) * BLK)
            hq[:, span] = hide(block, dot(fr[1], qf[:, span]))
        got(wdt, s_dp)
        for block in range(NBLK):
            settle(block, hq[:, block * BLK : (block + 1) * BLK])

    @pl.when(c == 1)
    def _():
        for block in range(NBLK):
            span = slice(block * BLK, (block + 1) * BLK)
            ql[:, span] = dot(fr[1], qf[:, span])
        lent()
        for block in range(NBLK):
            settle(block, hide(block, ql[:, block * BLK : (block + 1) * BLK]))

    def drain(ref, index):
        remote(ref, ref, snd.at[index], s_or, partner).wait_send()

    for block in range(NBLK):
        span = slice(block * BLK, (block + 1) * BLK)
        local(ro.at[own, span], ro.at[own, span], s_loc.at[5 + block]).wait()
    local(ao.at[own, :], att.at[:, half], s_loc.at[4]).wait()
    give.wait_send()
    got(ao.at[own, :], s_oa)
    for copy in lends:
        copy.wait_send()
    for copy in share:
        copy.wait_send()

    @pl.when(c == 0)
    def _():
        for copy in within:
            copy.wait_send()

    @pl.when((c == 1) & (y == 0))
    def _():
        for copy in cached:
            copy.wait_send()

    @pl.when(y < 3)
    def _():
        for copy in halo:
            copy.wait_send()

    @pl.when(source)
    def _():
        drain(kf.at[0:288, :], 0)
        drain(wm.at[0:192, :], 6)

    for index in range(2):
        drain(kf.at[0:256, :], 8 + index)
    drain(kf.at[0:256, :], 14)
    drain(kf.at[0:256, :], 10)
    drain(kf.at[0:128, :], 7)

    @pl.when(jnp.logical_not(source))
    def _():
        for copy in weight_share:
            copy.wait_send()
        drain(wm.at[0:256, :], 16)
        drain(wm.at[0:128, :], 21)
        drain(wdr.at[own, :], 22)

    drain(pr.at[main, :], 15)
    drain(rr.at[0:3, 0:32], 17)
    drain(ym.at[0:15], 18)

    @pl.when(c == 0)
    def _():
        drain(pr.at[down, :], 28)

    @pl.when(c == 1)
    def _():
        drain(rr.at[0:3, 32:64], 27)
        drain(yd.at[0:15], 19)
        lend_down.wait_send()

    drain(ro.at[0:64, :], 24)
    got(ro.at[0:64, :], s_or)


def write_out(att, rec, att_out, rec_out, sem):
    copies = [local(att, att_out, sem.at[0]), local(rec, rec_out, sem.at[1])]
    for copy in copies:
        copy.start()
    for copy in copies:
        copy.wait()


def per_device(*arrays):
    any_spec = pl.BlockSpec(memory_space=pl.ANY)
    out = pltpu.VMEM((64, 2 * HALF), BF16)
    arrays = [pltpu.with_memory_space_constraint(a, pltpu.HBM) for a in arrays]
    vmem = pltpu.VMEM
    dma = pltpu.SemaphoreType.DMA
    held = pl.pallas_call(
        kernel,
        out_shape=(out, out),
        in_specs=[any_spec] * 9,
        out_specs=(any_spec, any_spec),
        scratch_shapes=[
            vmem((512, HALF), BF16),
            vmem((512, HALF), BF16),
            vmem((512, HALF), BF16),
            vmem((128, HALF), BF16),
            vmem((128, HALF), BF16),
            vmem((512, 512), BF16),
            vmem((256, 512), BF16),
            vmem((512, 128), BF16),
            vmem((128, 512), BF16),
            vmem((128, 512), BF16),
            vmem((2 * HALF, 128), BF16),
            vmem((5 * BLK, BLK), F32),
            vmem((128, HALF), BF16),
            vmem((384, 512), F32),
            vmem((256, 512), BF16),
            vmem((256, 512), BF16),
            vmem((4, 64, 512), BF16),
            vmem((4, 64, 512), BF16),
            vmem((16, 32, 512), BF16),
            vmem((16, 32, 512), BF16),
            vmem((512, 512), BF16),
            vmem((512, 512), BF16),
            vmem((256, 512), F32),
            vmem((2, 512, 512), BF16),
            vmem((512, 512), BF16),
            vmem((128, HALF), BF16),
            vmem((8, HALF), F32),
            vmem((512, HALF), BF16),
            vmem((512, HALF), F32),
            dma((9,)),
            dma((2, 2)),
            dma((3,)),
            dma((2, NBLK, 2)),
            dma((2, NBLK)),
            dma((4,)),
            dma((3,)),
            dma((2,)),
            dma((2,)),
            dma((2,)),
            dma((2,)),
            dma((2,)),
            dma((2,)),
            dma((2, 4)),
            dma(()),
            dma((2, 4)),
            dma(()),
            dma(()),
            dma((2,)),
            dma(()),
            dma(()),
            dma((30,)),
        ],
        compiler_params=pltpu.CompilerParams(
            collective_id=0, has_side_effects=True, vmem_limit_bytes=48000000
        ),
        name="plane",
    )(*arrays)
    return pl.pallas_call(
        write_out,
        out_shape=(pltpu.HBM((64, 2 * HALF), BF16),) * 2,
        in_specs=[pl.BlockSpec(memory_space=vmem)] * 2,
        out_specs=(pl.BlockSpec(memory_space=pltpu.HBM),) * 2,
        scratch_shapes=[dma((2,))],
        name="write_out",
    )(*[pltpu.with_memory_space_constraint(a, pltpu.VMEM) for a in held])


def solution(mesh):
    split = Mesh(mesh.devices.reshape(8, 4, 2, 4), ("z", "x", "c", "y"))
    tokens = P(WIDE, "y")
    heads = P("y", None, None)
    return jax.shard_map(
        per_device,
        mesh=split,
        in_specs=(tokens, tokens, tokens, P(WIDE), P(WIDE), heads, heads, heads, P()),
        out_specs=(tokens, tokens),
        check_vma=False,
    )
```
